512 devices in a mesh: section: 4 (over y_hi), dp: 128 (over z, x, y_lo, core).
Axes of the slice: x: 4, y: 8 (y_hi: 4, y_lo: 2; y = y_hi * 2 + y_lo), z: 8, core: 2. Of those that a mesh axis runs over, the one named last changes fastest.
Arguments:
- saved_inputs: bfloat16 [4, 2, 16384, 320], P('section', None, 'dp'), may hold values from -6 to 6
- timesteps: int32 [2, 16384], P(None, 'dp'), may hold values from 0 to 999
- time_table: bfloat16 [1000, 320], replicated, may hold values from -6 to 6
- skip_weight: bfloat16 [4, 320, 320], P('section'), may hold values from -0.3125 to 0.3125
- ff_in: bfloat16 [4, 1280, 320], P('section'), may hold values from -0.3125 to 0.3125
- ff_out: bfloat16 [4, 1280, 320], P('section'), may hold values from -0.15625 to 0.15625
- output_cotangent: bfloat16 [2, 16384, 320], P(None, 'dp'), may hold values from -6 to 6
Outputs:
- input_grads: bfloat16 [4, 2, 16384, 320], P('section', None, 'dp')
- skip_weight_grad: float32 [4, 102400], P('section', 'dp')
- ff_in_grad: float32 [4, 1280, 320], P('section', 'dp')
- ff_out_grad: float32 [4, 1280, 320], P('section', 'dp')
The draws below stay inside these ranges and needn't reach their ends.
All inputs are finite; a program needn't handle non-finite values.
Results may differ from the reference program's by a relative error of at most 0.01.
Values may be sent and summed in bfloat16 or wider, within the bound.
A program may use at most 128 MiB of HBM per device.

```python
import jax
import jax.numpy as jnp
from jax import lax

C = 320
F = 1280
NT = 1000
M = 2
ROWS = 16384
N_SECTION = 4


def touch_ends(values, own_key, low, largest):
    longest = values.shape.index(max(values.shape))
    spots = []
    for shift in (0, 1):
        where = [jax.random.randint(jax.random.fold_in(own_key, axis), (), 0, length) for axis, length in enumerate(values.shape)]
        where[longest] = (where[longest] + shift) % values.shape[longest]
        spots.append(tuple(where))
    return values.at[spots[0]].set(low).at[spots[1]].set(largest)


def block_levels(stream_key, shape, cuts, least, top_value):
    def one(axis_at, blocks):
        draws = jax.random.uniform(jax.random.fold_in(jax.random.fold_in(stream_key, 6), axis_at), (blocks,), jnp.float32, least / len(cuts), top_value / len(cuts))
        return jnp.repeat(jnp.exp(draws), shape[axis_at] // blocks).reshape((-1,) + (1,) * (len(shape) - axis_at - 1))

    gain = one(*cuts[0])
    for cut in cuts[1:]:
        gain = gain * one(*cut)
    return gain


def normal_values(stream_key, extent, spread, reach, shards=(), kind=jnp.bfloat16):
    array = spread * jax.random.normal(stream_key, extent, jnp.float32)
    if shards:
        array = array * block_levels(stream_key, extent, shards, -0.22, 0.18)
    return jnp.clip(array, -reach, reach).astype(kind)


def setup_inputs(seed: int = 0) -> dict:
    key_list = jax.random.split(jax.random.key(seed), 8)
    return {
        "saved_inputs": normal_values(key_list[0], (N_SECTION, M, ROWS, C), 1.0, 6.0, ((0, 4), (2, 128))),
        "timesteps": touch_ends(jax.random.randint(key_list[1], (M, ROWS), 0, NT), jax.random.fold_in(key_list[1], 1), 0, NT - 1).astype(jnp.int32),
        "time_table": normal_values(key_list[2], (NT, C), 1.0, 6.0),
        "skip_weight": normal_values(key_list[3], (N_SECTION, C, C), C ** -0.5, 0.3125, ((0, 4),)),
        "ff_in": normal_values(key_list[4], (N_SECTION, F, C), C ** -0.5, 0.3125, ((0, 4),)),
        "ff_out": normal_values(key_list[5], (N_SECTION, F, C), F ** -0.5, 0.15625, ((0, 4),)),
        "output_cotangent": normal_values(key_list[6], (M, ROWS, C), 1.0, 6.0, ((1, 128),)),
    }


EPS = 1e-06

def contract(left, right, dims):
    return lax.dot_general(left, right, ((dims[0], dims[1]), ((), ())), preferred_element_type=jnp.float32)

def forward(inputs, source, w_skip, w_in, w_out):
    united = inputs.astype(jnp.float32) + jnp.dot(source, w_skip, preferred_element_type=jnp.float32)
    recip = lax.rsqrt(lax.optimization_barrier(jnp.mean(united * united, axis=-1, keepdims=True)) + EPS)
    normed = (united * recip).astype(jnp.bfloat16)
    preact = contract(normed, w_in, ((1,), (1,)))
    active = jax.nn.silu(preact).astype(jnp.bfloat16)
    output = united + jnp.dot(active, w_out, preferred_element_type=jnp.float32)
    return (united, recip, normed, preact, active, output)

def backward(grad_out, inputs, source, w_skip, w_in, w_out):
    united, recip, normed, preact, active, output = forward(inputs, source, w_skip, w_in, w_out)
    grad_low = grad_out.astype(jnp.bfloat16)
    grad_act = contract(grad_low, w_out, ((1,), (1,)))
    sigma = jax.nn.sigmoid(preact)
    grad_pre = (grad_act * sigma * (1.0 + preact * (1.0 - sigma))).astype(jnp.bfloat16)
    d_in = contract(grad_pre, normed, ((0,), (0,)))
    d_out = contract(active, grad_low, ((0,), (0,)))
    grad_norm = jnp.dot(grad_pre, w_in, preferred_element_type=jnp.float32)
    grad_united = grad_out + recip * grad_norm - united * recip ** 3 * lax.optimization_barrier(jnp.mean(grad_norm * united, axis=-1, keepdims=True))
    united_low = grad_united.astype(jnp.bfloat16)
    d_skip = contract(source, united_low, ((0,), (0,)))
    grad_source = contract(united_low, w_skip, ((1,), (1,))).astype(jnp.bfloat16)
    return (united_low, grad_source, d_in, d_out, d_skip)

def reference(saved_inputs, timesteps, time_table, skip_weight, ff_in, ff_out, output_cotangent):
    grads = [[None] * M for section in range(4)]
    sum_in = [jnp.zeros((F, C), jnp.float32) for section in range(4)]
    sum_out = [jnp.zeros((F, C), jnp.float32) for section in range(4)]
    sum_skip = [jnp.zeros((C, C), jnp.float32) for section in range(4)]
    for micro in range(M):
        embeds = jnp.take(time_table, timesteps[micro], axis=0)
        values = []
        for section in range(2):
            output = forward(saved_inputs[section, micro], embeds, skip_weight[section], ff_in[section], ff_out[section])[5]
            values.append(output.astype(jnp.bfloat16))
        pending = [None, None]
        chain = None
        for section in (3, 2, 1, 0):
            if section == 3:
                grad_out = output_cotangent[micro].astype(jnp.float32)
            elif section == 2:
                grad_out = chain.astype(jnp.float32)
            else:
                grad_out = chain.astype(jnp.float32) + pending[section].astype(jnp.float32)
            source = values[3 - section] if section >= 2 else embeds
            parts = backward(grad_out, saved_inputs[section, micro], source, skip_weight[section], ff_in[section], ff_out[section])
            chain = parts[0]
            if section >= 2:
                pending[3 - section] = parts[1]
            grads[section][micro] = chain
            sum_in[section] = sum_in[section] + parts[2]
            sum_out[section] = sum_out[section] + parts[3]
            sum_skip[section] = sum_skip[section] + parts[4]
    input_grads = jnp.stack([jnp.stack(grads[section]) for section in range(4)])
    skip_grad = jnp.stack([sum_skip[section].reshape(-1) for section in range(4)])
    return (input_grads, skip_grad, jnp.stack(sum_in), jnp.stack(sum_out))
```

```python
import jax
import jax.numpy as jnp
from jax import lax
from jax.experimental import pallas as pl
from jax.experimental.pallas import tpu as pltpu
from jax.sharding import Mesh
from jax.sharding import PartitionSpec as P

DP = ("z", "x", "w", "core")
MESH = pl.DeviceIdType.MESH
EPS = 1e-06
CHUNKS = 4
F32 = jnp.float32
BF16 = jnp.bfloat16


def dot(left, right):
    return jnp.dot(left, right, preferred_element_type=F32)


def dot_nt(left, right):
    return lax.dot_general(left, right, (((1,), (1,)), ((), ())), preferred_element_type=F32)


def dot_tn(left, right):
    return lax.dot_general(left, right, (((0,), (0,)), ((), ())), preferred_element_type=F32)


def chain_kernel(
    x_ref,
    ts_ref,
    table_ref,
    wskip_ref,
    win_ref,
    wout_ref,
    cot_ref,
    grads_ref,
    din_ref,
    dout_ref,
    dskip_ref,
    z_buf,
    g_buf,
    k_buf,
    vsend,
    csend,
    ksend,
    u_buf,
    r_buf,
    n_buf,
    act_buf,
    ds_buf,
    gpre_buf,
    gyb_buf,
    vs_sem,
    vr_sem,
    cs_sem,
    cr_sem,
    ks_sem,
    kr_sem,
):
    section = lax.axis_index("section")
    rows = x_ref.shape[0] // CHUNKS
    micro, per = ts_ref.shape
    levels = table_ref.shape[0]

    barrier = pltpu.get_barrier_semaphore()
    for step in (1, 3):
        pl.semaphore_signal(
            barrier, inc=1, device_id={"section": lax.rem(section + step, 4)}, device_id_type=MESH
        )
    pl.semaphore_wait(barrier, 2)

    def at(c):
        return pl.ds(pl.multiple_of(c * rows, rows), rows)

    def value_copy(c):
        return pltpu.make_async_remote_copy(
            src_ref=vsend.at[at(c)],
            dst_ref=z_buf.at[at(c)],
            send_sem=vs_sem.at[c],
            recv_sem=vr_sem.at[c],
            device_id={"section": 3 - section},
            device_id_type=MESH,
        )

    def chain_copy(c):
        return pltpu.make_async_remote_copy(
            src_ref=csend.at[at(c)],
            dst_ref=g_buf.at[at(c)],
            send_sem=cs_sem.at[c],
            recv_sem=cr_sem.at[c],
            device_id={"section": lax.rem(section + 3, 4)},
            device_id_type=MESH,
        )

    def skip_copy(c):
        return pltpu.make_async_remote_copy(
            src_ref=ksend.at[at(c)],
            dst_ref=k_buf.at[at(c)],
            send_sem=ks_sem.at[c],
            recv_sem=kr_sem.at[c],
            device_id={"section": lax.rem(section + 1, 4)},
            device_id_type=MESH,
        )

    def forward(c, encoder):
        here = at(c)
        united = x_ref[here, :].astype(F32) + dot(z_buf[here, :], wskip_ref[...])
        recip = lax.rsqrt(jnp.mean(united * united, axis=-1, keepdims=True) + EPS)
        normed = (united * recip).astype(BF16)
        preact = dot_nt(normed, win_ref[...])
        sigma = jax.nn.sigmoid(preact)
        active = (preact * sigma).astype(BF16)
        u_buf[here, :] = united
        r_buf[here, :] = jnp.broadcast_to(recip, (rows, 128))
        n_buf[here, :] = normed
        act_buf[here, :] = active
        ds_buf[here, :] = sigma * (1.0 + preact * (1.0 - sigma))
        if encoder:
            vsend[here, :] = (united + dot(active, wout_ref[...])).astype(BF16)
            value_copy(c).start()

    def backward(c):
        here = at(c)
        gy = g_buf[here, :].astype(F32) + k_buf[here, :].astype(F32)
        low = gy.astype(BF16)
        gyb_buf[here, :] = low
        pre = (dot_nt(low, wout_ref[...]) * ds_buf[here, :]).astype(BF16)
        gpre_buf[here, :] = pre
        gn = dot(pre, win_ref[...])
        united = u_buf[here, :]
        recip = r_buf[here, 0:1]
        mean = jnp.mean(gn * united, axis=-1, keepdims=True)
        chain = (gy + recip * gn - united * (recip * recip * recip * mean)).astype(BF16)
        grads_ref[here, :] = chain

        @pl.when(section == 1)
        def _():
            csend[here, :] = chain

        @pl.when(section >= 2)
        def _():
            back = dot_nt(chain, wskip_ref[...]).astype(BF16)

            @pl.when(section == 2)
            def _():
                csend[here, :] = (chain.astype(F32) + back.astype(F32)).astype(BF16)

            @pl.when(section == 3)
            def _():
                csend[here, :] = chain
                ksend[here, :] = back
                skip_copy(c).start()

        @pl.when(section > 0)
        def _():
            chain_copy(c).start()

    @pl.when(section > 0)
    def _():
        k_buf[...] = jnp.zeros_like(k_buf)

    @pl.when(section < 2)
    def _():
        for m in range(micro):
            column = jnp.broadcast_to(ts_ref[m : m + 1, :].astype(F32), (per, per)).T
            onehot = column[:, 0:1] == lax.broadcasted_iota(jnp.int32, (per, levels), 1).astype(F32)
            z_buf[m * per : (m + 1) * per, :] = dot(
                jnp.where(onehot, 1.0, 0.0).astype(BF16), table_ref[...]
            ).astype(BF16)

        @pl.loop(0, CHUNKS)
        def _(c):
            forward(c, True)

    @pl.when(section == 3)
    def _():
        g_buf[...] = cot_ref[...]

    @pl.when(section >= 2)
    def _():
        @pl.loop(0, CHUNKS)
        def _(c):
            value_copy(c).wait_recv()
            forward(c, False)

            @pl.when(section == 3)
            def _():
                backward(c)

    @pl.when(section < 3)
    def _():
        @pl.loop(0, CHUNKS)
        def _(c):
            chain_copy(c).wait_recv()

            @pl.when(section == 0)
            def _():
                skip_copy(c).wait_recv()

            backward(c)

    dout_ref[...] = dot_tn(act_buf[...], gyb_buf[...]).astype(BF16)
    din_ref[...] = dot_tn(gpre_buf[...], n_buf[...]).astype(BF16)
    dskip_ref[...] = dot_tn(z_buf[...], grads_ref[...]).astype(BF16)

    for c in range(CHUNKS):

        @pl.when(section < 2)
        def _():
            value_copy(c).wait_send()

        @pl.when(section > 0)
        def _():
            chain_copy(c).wait_send()

        @pl.when(section == 3)
        def _():
            skip_copy(c).wait_send()


def cut_along(shard, dim, length):
    before, after = (shard.shape[:dim], shard.shape[dim + 1 :])
    return jnp.moveaxis(shard.reshape(*before, length, -1, *after), dim, 0)


def sum_at_owner(shard, axis, dim):
    length = lax.axis_size(axis)
    blocks = lax.all_to_all(cut_along(shard, dim, length), axis, 0, 0, tiled=True)
    return jnp.sum(blocks.astype(jnp.float32), axis=0)


def sum_by_axis(shard, axes, dim):
    far, near = axes
    own = sum_at_owner(cut_along(shard, dim, lax.axis_size(far)), near, dim + 1)
    return jnp.sum(
        lax.all_to_all(own.astype(jnp.bfloat16), far, 0, 0, tiled=True).astype(jnp.float32), axis=0
    )


def sent_together(arrays, axis, dim, along):
    ends, at = ([], 0)
    for a in arrays[:-1]:
        at += a.shape[along]
        ends.append(at)
    both = jnp.concatenate(arrays, axis=along)
    return tuple(jnp.split(sum_by_axis(both, axis, dim), ends, axis=along))


def shards(saved_inputs, timesteps, time_table, skip_weight, ff_in, ff_out, output_cotangent):
    n_micro, per, width = saved_inputs.shape[1:]
    hidden = ff_in.shape[1]
    total = n_micro * per
    low = pltpu.VMEM((total, width), BF16)
    grads, d_in, d_out, d_skip = pl.pallas_call(
        chain_kernel,
        out_shape=(
            jax.ShapeDtypeStruct((total, width), BF16),
            jax.ShapeDtypeStruct((hidden, width), BF16),
            jax.ShapeDtypeStruct((hidden, width), BF16),
            jax.ShapeDtypeStruct((width, width), BF16),
        ),
        in_specs=[pl.BlockSpec(memory_space=pltpu.VMEM)] * 7,
        out_specs=(pl.BlockSpec(memory_space=pltpu.VMEM),) * 4,
        scratch_shapes=[
            low,
            low,
            low,
            low,
            low,
            low,
            pltpu.VMEM((total, width), F32),
            pltpu.VMEM((total, 128), F32),
            low,
            pltpu.VMEM((total, hidden), BF16),
            pltpu.VMEM((total, hidden), F32),
            pltpu.VMEM((total, hidden), BF16),
            low,
        ]
        + [pltpu.SemaphoreType.DMA((CHUNKS,))] * 6,
        compiler_params=pltpu.CompilerParams(collective_id=0, has_side_effects=True),
    )(
        saved_inputs.reshape(total, width),
        timesteps,
        time_table,
        skip_weight[0],
        ff_in[0],
        ff_out[0],
        output_cotangent.reshape(total, width),
    )
    axes = (("z", "x", "w"), "core")
    grad_in, grad_out = sent_together((d_in, d_out), axes, 0, 1)
    grad_skip = sum_by_axis(d_skip.reshape(-1), axes, 0)
    return (grads.reshape(1, n_micro, per, width), grad_skip[None], grad_in[None], grad_out[None])


def solution(mesh):
    split = Mesh(
        mesh.devices.reshape(mesh.shape["section"], 8, 4, 2, 2), ("section", "z", "x", "w", "core")
    )
    return jax.shard_map(
        shards,
        mesh=split,
        in_specs=(
            P("section", None, DP, None),
            P(None, DP),
            P(),
            P("section", None, None),
            P("section", None, None),
            P("section", None, None),
            P(None, DP, None),
        ),
        out_specs=(
            P("section", None, DP, None),
            P("section", DP),
            P("section", DP, None),
            P("section", DP, None),
        ),
        check_vma=False,
    )
```

```python
import jax
import jax.numpy as jnp
from jax import lax
from jax.experimental import pallas as pl
from jax.experimental.pallas import tpu as pltpu
from jax.sharding import Mesh
from jax.sharding import PartitionSpec as P

DP = ("z", "x", "w", "core")
MESH = pl.DeviceIdType.MESH
EPS = 1e-06
CHUNKS = 8
LAG = 4
FF_ROWS = 40
BLOCK = 48
PIECE = 16
F32 = jnp.float32
BF16 = jnp.bfloat16


def dot(left, right):
    return jnp.dot(left, right, preferred_element_type=F32)


def dot_nt(left, right):
    return lax.dot_general(left, right, (((1,), (1,)), ((), ())), preferred_element_type=F32)


def kernel(
    xt_hbm,
    ts_hbm,
    tablet_hbm,
    wskip_hbm,
    wint_hbm,
    woutt_hbm,
    cott_hbm,
    grads_ref,
    din_ref,
    dout_ref,
    dskip_ref,
    xt_ref,
    ts_ref,
    tablet_ref,
    wskip_ref,
    wint_ref,
    woutt_ref,
    cott_ref,
    in_sem,
    ga_buf,
    v_msg,
    g_msg,
    k_msg,
    x_buf,
    z_buf,
    g_buf,
    vsend,
    csend,
    ksend,
    u_buf,
    r_buf,
    ds_buf,
    ch_buf,
    chsh_buf,
    nq,
    gq,
    sel,
    win_q,
    wout_q,
    act_t,
    ds_q,
    gpre_t,
    za_t,
    zb_t,
    skip_part,
    skip_core,
    skip_w,
    part,
    r_x1,
    r_x2,
    z_send,
    r_z,
    vs_sem,
    vr_sem,
    cs_sem,
    cr_sem,
    ks_sem,
    kr_sem,
    n_s,
    n_r,
    gs_s,
    gs_r,
    sk_s,
    sk_r,
    x1_s,
    x1_r,
    x1k_s,
    x1k_r,
    x2_s,
    x2_r,
    z_s,
    z_r,
):
    section = lax.axis_index("section")
    mz = lax.axis_index("z")
    mx = lax.axis_index("x")
    mw = lax.axis_index("w")
    mc = lax.axis_index("core")
    pairs = (
        (ts_hbm, ts_ref),
        (tablet_hbm, tablet_ref),
        (xt_hbm, xt_ref),
        (wskip_hbm, wskip_ref),
        (wint_hbm, wint_ref),
        (woutt_hbm, woutt_ref),
        (cott_hbm, cott_ref),
    )
    loads = [pltpu.make_async_copy(a, b, in_sem.at[i]) for i, (a, b) in enumerate(pairs)]
    for load in loads:
        load.start()
    micro, width, per = xt_ref.shape
    total = micro * per
    rows = total // CHUNKS
    levels = tablet_ref.shape[1]
    hidden = wint_ref.shape[1]

    def remote(src, dst, send, recv, device):
        return pltpu.make_async_remote_copy(
            src_ref=src,
            dst_ref=dst,
            send_sem=send,
            recv_sem=recv,
            device_id=device,
            device_id_type=MESH,
        )

    x_near = mx + 1 - 2 * lax.rem(mx, 2)
    x_far = 3 - mx
    x_op = lax.rem(mx + 2, 4)

    barrier = pltpu.get_barrier_semaphore()
    greet = [{"section": lax.rem(section + step, 4)} for step in (1, 3)]
    greet += [{"core": 1 - mc}, {"x": x_near}, {"x": x_far}, {"w": 1 - mw}]
    greet += [{"z": lax.rem(mz + step, 8)} for step in range(1, 8)]
    for device in greet:
        pl.semaphore_signal(barrier, inc=1, device_id=device, device_id_type=MESH)
    pl.semaphore_wait(barrier, len(greet))

    def at(c):
        return pl.ds(pl.multiple_of(c * rows, rows), rows)

    def value_copy(c):
        device = {"section": 3 - section}
        return remote(vsend.at[c], v_msg.at[c], vs_sem.at[c], vr_sem.at[c], device)

    def chain_copy(c):
        device = {"section": lax.rem(section + 3, 4)}
        return remote(csend.at[c], g_msg.at[c], cs_sem.at[c], cr_sem.at[c], device)

    def skip_copy(c):
        device = {"section": lax.rem(section + 1, 4)}
        return remote(ksend.at[c], k_msg.at[c], ks_sem.at[c], kr_sem.at[c], device)

    def paced(copy, c):
        @pl.when(c >= 2)
        def _():
            copy(c - 2).wait_send()

        copy(c).start()

    rest = width - 256
    short = rows // 2

    def pack(buf, c, value):
        value = value.astype(BF16)
        buf[c, 0:rows, :] = value[:, 0:128]
        buf[c, rows : 2 * rows, :] = value[:, 128:256]
        buf[c, 2 * rows :, 0:rest] = value[0:short, 256:width]
        buf[c, 2 * rows :, rest:] = value[short:, 256:width]

    def unpack(buf, c):
        tail = jnp.concatenate([buf[c, 2 * rows :, 0:rest], buf[c, 2 * rows :, rest:]], axis=0)
        return jnp.concatenate([buf[c, 0:rows, :], buf[c, rows : 2 * rows, :], tail], axis=1)

    def forward(c, kind):
        here = at(c)
        if kind == "decoder":
            value_copy(c).wait_recv()
            z_buf[here, :] = unpack(v_msg, c)
        united = x_buf[here, :] + dot(z_buf[here, :], wskip_ref[...])
        recip = lax.rsqrt(jnp.mean(united * united, axis=-1, keepdims=True) + EPS)
        normed = (united * recip).astype(BF16)
        preact = dot(normed, wint_ref[...])
        sigma = jax.nn.sigmoid(preact)
        active = (preact * sigma).astype(BF16)
        if kind == "encoder":
            pack(vsend, c, united + dot_nt(active, woutt_ref[...]))
            paced(value_copy, c)
        u_buf[here, :] = united
        r_buf[here, :] = jnp.broadcast_to(recip, (rows, 128))
        nq[me, here, 0:width] = normed
        ds_buf[here, :] = sigma * (1.0 + preact * (1.0 - sigma))

    def finish(c, gy, low, gact):
        here = at(c)
        pre = (gact * ds_buf[here, :]).astype(BF16)
        gn = dot_nt(pre, wint_ref[...])
        united = u_buf[here, :]
        recip = r_buf[here, 0:1]
        mean = jnp.mean(gn * united, axis=-1, keepdims=True)
        chain = gy + recip * gn - united * (recip * recip * recip * mean)
        low_chain = chain.astype(BF16)
        ch_buf[here, 0:width] = low_chain
        chsh_buf[here, 64 : 64 + width] = low_chain
        return low_chain

    def backward(c, which):
        here = at(c)
        if which == 3:
            low = g_buf[here, :]
            chain = finish(c, low.astype(F32), low, ga_buf[here, :])
            pack(csend, c, chain)
            paced(chain_copy, c)
            pack(ksend, c, dot_nt(chain, wskip_ref[...]))
            paced(skip_copy, c)
            return
        chain_copy(c).wait_recv()
        gy = unpack(g_msg, c).astype(F32)
        if which == 0:
            skip_copy(c).wait_recv()
            gy = gy + unpack(k_msg, c).astype(F32)
        low = gy.astype(BF16)
        gq[me, here, 64 : 64 + width] = low
        if which == 0:
            for to in range(2):
                share_g(c, to).start()
        chain = finish(c, gy, low, dot(low, woutt_ref[...]))
        if which == 2:
            back = dot_nt(chain, wskip_ref[...]).astype(BF16)
            pack(csend, c, chain.astype(F32) + back.astype(F32))
        if which == 1:
            pack(csend, c, chain)
        if which > 0:
            paced(chain_copy, c)

    me = 2 * mw + mc
    mates = (2 * mw + 1 - mc, 2 * (1 - mw) + mc, 2 * (1 - mw) + 1 - mc)
    towards = ({"core": 1 - mc}, {"w": 1 - mw}, {"core": 1 - mc})

    def share_n(to):
        slot = mates[1] if to == 2 else me
        return remote(nq.at[slot], nq.at[slot], n_s.at[to], n_r.at[to], towards[to])

    def share_g(c, to):
        slot = mates[1] if to == 2 else me
        block = gq.at[slot, at(c)]
        return remote(block, block, gs_s.at[to, c], gs_r.at[to, c], towards[to])

    nq[me, :, width:] = jnp.zeros((total, 384 - width), BF16)
    gq[me, :, 0:64] = jnp.zeros((total, 64), BF16)
    ch_buf[:, width:] = jnp.zeros((total, 384 - width), BF16)
    chsh_buf[:, 0:64] = jnp.zeros((total, 64), BF16)

    def rows_of(m):
        return slice(m * per, (m + 1) * per)

    @pl.when(section < 2)
    def _():
        for load in loads[0:2]:
            load.wait()
        for m in range(micro):
            onehot = ts_ref[m : m + 1, :] == lax.broadcasted_iota(jnp.int32, (levels, per), 0)
            embed = dot(tablet_ref[...], jnp.where(onehot, 1.0, 0.0).astype(BF16))
            z_buf[rows_of(m), :] = embed.T.astype(BF16)

    loads[2].wait()
    for m in range(micro):
        x_buf[rows_of(m), :] = xt_ref[m].astype(F32).T
    for load in loads[3:]:
        load.wait()

    @pl.when(section < 2)
    def _():
        @pl.loop(0, CHUNKS)
        def _(c):
            forward(c, "encoder")

    @pl.when(section >= 2)
    def _():
        for load in loads[0:2]:
            load.wait()

    @pl.when(section == 3)
    def _():
        for m in range(micro):
            cot = cott_ref[m].astype(F32).T.astype(BF16)
            g_buf[rows_of(m), :] = cot
            gq[me, rows_of(m), 64 : 64 + width] = cot
        ga_buf[...] = dot(g_buf[...], woutt_ref[...])

        @pl.loop(0, CHUNKS)
        def _(c):
            forward(c, "decoder")
            backward(c, 3)

    @pl.when(section == 2)
    def _():
        @pl.loop(0, CHUNKS + LAG)
        def _(t):
            @pl.when(t < CHUNKS)
            def _():
                forward(t, "decoder")

            @pl.when(t >= LAG)
            def _():
                backward(t - LAG, 2)

    for to in range(2):
        share_n(to).start()
    line = lax.broadcasted_iota(jnp.int32, (hidden, width), 1)
    unit = 40 * (4 * (lax.rem(line, 80) // 10) + line // 80) + 10 * me + lax.rem(line, 10)
    chosen = lax.broadcasted_iota(jnp.int32, (hidden, width), 0) == unit
    sel[...] = jnp.where(chosen, 1.0, 0.0).astype(BF16)
    win_q[...] = dot(wint_ref[...], sel[...]).astype(BF16)
    wout_q[0:64, :] = jnp.zeros((64, width), BF16)
    wout_q[64:, :] = dot(woutt_ref[...], sel[...]).astype(BF16)
    slot = lax.broadcasted_iota(jnp.int32, (256, width), 0)
    channel = lax.broadcasted_iota(jnp.int32, (256, width), 1)
    third = lax.rem(slot, 2)
    pixel = lax.rem(slot, 64) // 2
    first = 10 * (4 * lax.rem(pixel, 8) + pixel // 8) + 5 * lax.rem(slot // 64, 2)
    first = first + 2 * (slot // 128)
    for dst, pick in (
        (za_t, channel == first + 2 * third),
        (zb_t, (channel == first + 1) & (third == 0)),
    ):
        dst[...] = dot_nt(jnp.where(pick, 1.0, 0.0).astype(BF16), z_buf[...]).astype(BF16)
    share_n(1).wait_recv()
    share_n(2).start()
    share_n(0).wait_recv()
    share_n(2).wait_recv()

    @pl.loop(0, 4)
    def _(q):
        preact = dot(nq[q, :, 0:width], win_q[...])
        sigma = jax.nn.sigmoid(preact)
        ds_q[q] = sigma * (1.0 + preact * (1.0 - sigma))
        act_t[:, pl.ds(pl.multiple_of(q * total, total), total)] = (preact * sigma).astype(BF16).T

    for which in (0, 1):

        @pl.when(section == which)
        def _():
            @pl.loop(0, CHUNKS)
            def _(c):
                backward(c, which)

    def joined(left, right):
        return left[:, 0:256], left[:, 256:384] + right[:, 0:128], right[:, 128:384]

    edges = (slice(0, 256), slice(256, 384), slice(384, 640))

    @pl.when(section > 0)
    def _():
        @pl.loop(0, CHUNKS)
        def _(c):
            for to in range(2):
                share_g(c, to).start()

    skips = joined(dot(za_t[...], ch_buf[...]), dot(zb_t[...], chsh_buf[...]))
    for edge, value in zip(edges, skips):
        skip_part[:, :, :, edge] = value.astype(BF16).reshape(2, 2, 64, -1)
    skip1 = remote(skip_part.at[1 - mc], skip_core, sk_s.at[0], sk_r.at[0], {"core": 1 - mc})
    skip2 = remote(skip_part.at[mc, 1 - mw], skip_w, sk_s.at[1], sk_r.at[1], {"w": 1 - mw})
    skip1.start()

    @pl.loop(0, CHUNKS)
    def _(c):
        share_g(c, 1).wait_recv()
        share_g(c, 2).start()

    skip1.wait_recv()
    other = skip_part[mc, 1 - mw].astype(F32) + skip_core[1 - mw].astype(F32)
    skip_part[mc, 1 - mw] = other.astype(BF16)
    skip2.start()
    own_skip = skip_part[mc, mw].astype(F32) + skip_core[mw].astype(F32)
    skip_part[mc, mw] = own_skip.astype(BF16)

    def through(q):
        pre = (dot(gq[q], wout_q[...]) * ds_q[q]).astype(BF16)
        gpre_t[:, pl.ds(pl.multiple_of(q * total, total), total)] = pre.T

    through(me)
    through(mates[1])
    for to in (0, 2):

        @pl.loop(0, CHUNKS)
        def _(c):
            share_g(c, to).wait_recv()

        through(mates[to])

    everyone = 4 * total
    d_out = dot(act_t[...], gq[...].reshape(everyone, 384))
    d_in = dot(gpre_t[...], nq[...].reshape(everyone, 384))
    for edge, value in zip(edges, joined(d_in, d_out)):
        value = value.astype(BF16).reshape(4, 2, FF_ROWS, -1)
        for color in range(2):
            part[color, :, 0:FF_ROWS, edge] = value[:, color]

    def x1_block(color, k):
        device = x_far if color else x_near
        return device, device if k == 0 else x_op

    def x1_copy(color, k):
        device, block = x1_block(color, k)
        span = pl.ds(0, FF_ROWS)
        src, dst = part.at[color, block, span], r_x1.at[color, k, span]
        return remote(src, dst, x1_s.at[color, k], x1_r.at[color, k], {"x": device})

    def x1k_copy(color, k):
        device, block = x1_block(color, k)
        span = pl.ds(FF_ROWS, BLOCK - FF_ROWS)
        src, dst = part.at[color, block, span], r_x1.at[color, k, span]
        return remote(src, dst, x1k_s.at[color, k], x1k_r.at[color, k], {"x": device})

    def x2_copy(color):
        device = x_near if color else x_far
        src = part.at[color, device]
        return remote(src, r_x2.at[color], x2_s.at[color], x2_r.at[color], {"x": device})

    for k in (1, 0):
        for color in range(2):
            x1_copy(color, k).start()
    skip2.wait_recv()
    own = (skip_part[mc, mw].astype(F32) + skip_w[...].astype(F32)).astype(BF16)
    own = own.reshape(4, 2, BLOCK - FF_ROWS, 2 * width)
    for color in range(2):
        part[color, :, FF_ROWS:, :] = own[:, color]
    for k in (1, 0):
        for color in range(2):
            x1k_copy(color, k).start()
    for m in range(micro):
        grads_ref[m] = ch_buf[m * per : (m + 1) * per, 0:width].astype(F32).T.astype(BF16)

    def added(left, right):
        return left.astype(F32) + right.astype(F32)

    for color in range(2):
        other = x_near if color else x_far
        for k in (1, 0):
            x1_copy(color, k).wait_recv()
            x1k_copy(color, k).wait_recv()
            block = other if k == 1 else mx
            part[color, block] = added(part[color, block], r_x1[color, k]).astype(BF16)
            if k == 1:
                x2_copy(color).start()

    def z_copy(k):
        target = lax.rem(mz + k, 8)
        return remote(z_send.at[target], r_z.at[mz], z_s.at[k], z_r.at[mz], {"z": target})

    for color in range(2):
        x2_copy(color).wait_recv()
        block = added(part[color, mx], r_x2[color])
        for j in range(4):
            piece = (
                block[10 * j : 10 * j + 10],
                block[FF_ROWS + 2 * j : FF_ROWS + 2 * j + 2],
                jnp.zeros((PIECE - 12, 2 * width), F32),
            )
            z_send[4 * color + j] = jnp.concatenate(piece, axis=0).astype(BF16)
    far_first = (4, 3, 5, 2, 6, 1, 7)
    for k in far_first:
        z_copy(k).start()
    acc = z_send[mz].astype(F32)
    for k in reversed(far_first):
        source = lax.rem(mz + 8 - k, 8)
        slot = r_z.at[source]
        remote(slot, slot, z_s.at[k], z_r.at[source], {"z": source}).wait_recv()
        acc = acc + r_z[source].astype(F32)

    for j in range(10):
        din_ref[j] = acc[j : j + 1, 0:width]
        dout_ref[j] = acc[j : j + 1, width:]
    half = width // 2
    lead, mid, last = acc[10:11, 0:width], acc[10:11, width:], acc[11:12, 0:width]

    @pl.when(mc == 0)
    def _():
        dskip_ref[:, 0:width] = lead
        dskip_ref[:, width : 2 * width] = mid
        dskip_ref[:, 2 * width :] = last[:, 0:half]

    @pl.when(mc == 1)
    def _():
        dskip_ref[:, 0:half] = lead[:, half:]
        dskip_ref[:, half : half + width] = mid
        dskip_ref[:, half + width :] = last

    for to in range(3):
        share_n(to).wait_send()
    skip1.wait_send()
    skip2.wait_send()

    @pl.loop(0, CHUNKS)
    def _(c):
        for to in range(3):
            share_g(c, to).wait_send()

    @pl.when(section < 2)
    def _():
        for late in range(1, 3):
            value_copy(CHUNKS - late).wait_send()

    @pl.when(section > 0)
    def _():
        for late in range(1, 3):
            chain_copy(CHUNKS - late).wait_send()

    @pl.when(section == 3)
    def _():
        for late in range(1, 3):
            skip_copy(CHUNKS - late).wait_send()

    for color in range(2):
        for k in range(2):
            x1_copy(color, k).wait_send()
            x1k_copy(color, k).wait_send()
        x2_copy(color).wait_send()
    for k in range(1, 8):
        z_copy(k).wait_send()


def finish(*refs):
    copies = [pltpu.make_async_copy(refs[i], refs[4 + i], refs[8].at[i]) for i in range(4)]
    for copy in copies:
        copy.start()
    for copy in copies:
        copy.wait()


def shards(saved_inputs, timesteps, time_table, skip_weight, ff_in, ff_out, output_cotangent):
    n_micro, per, width = saved_inputs.shape[1:]
    hidden = ff_in.shape[1]
    total = n_micro * per
    lanes = 2 * width
    shapes = (
        jax.ShapeDtypeStruct((n_micro, width, per), BF16),
        jax.ShapeDtypeStruct((10, 1, width), F32),
        jax.ShapeDtypeStruct((10, 1, width), F32),
        jax.ShapeDtypeStruct((1, 800), F32),
    )
    low = pltpu.VMEM((total, width), BF16)
    message = pltpu.VMEM((CHUNKS, total // CHUNKS * width // 128, 128), BF16)
    wide = pltpu.VMEM((total, 384), BF16)
    dma = pltpu.SemaphoreType.DMA
    held = pl.pallas_call(
        kernel,
        out_shape=tuple(pltpu.VMEM(s.shape, s.dtype) for s in shapes),
        in_specs=[pl.BlockSpec(memory_space=pl.ANY)] * 7,
        out_specs=(pl.BlockSpec(memory_space=pltpu.VMEM),) * 4,
        scratch_shapes=[
            pltpu.VMEM((n_micro, width, per), BF16),
            pltpu.VMEM(timesteps.shape, jnp.int32),
            pltpu.VMEM((width, time_table.shape[0]), BF16),
            pltpu.VMEM((width, width), BF16),
            pltpu.VMEM((width, hidden), BF16),
            pltpu.VMEM((width, hidden), BF16),
            pltpu.VMEM((n_micro, width, per), BF16),
            dma((7,)),
            pltpu.VMEM((total, hidden), F32),
            message,
            message,
            message,
            pltpu.VMEM((total, width), F32),
            low,
            low,
            message,
            message,
            message,
            pltpu.VMEM((total, width), F32),
            pltpu.VMEM((total, 128), F32),
            pltpu.VMEM((total, hidden), F32),
            wide,
            wide,
            pltpu.VMEM((4, total, 384), BF16),
            pltpu.VMEM((4, total, 384), BF16),
            pltpu.VMEM((hidden, width), BF16),
            pltpu.VMEM((width, width), BF16),
            pltpu.VMEM((384, width), BF16),
            pltpu.VMEM((width, 4 * total), BF16),
            pltpu.VMEM((4, total, width), F32),
            pltpu.VMEM((width, 4 * total), BF16),
            pltpu.VMEM((256, total), BF16),
            pltpu.VMEM((256, total), BF16),
            pltpu.VMEM((2, 2, 64, lanes), BF16),
            pltpu.VMEM((2, 64, lanes), BF16),
            pltpu.VMEM((64, lanes), BF16),
            pltpu.VMEM((2, 4, BLOCK, lanes), BF16),
            pltpu.VMEM((2, 2, BLOCK, lanes), BF16),
            pltpu.VMEM((2, BLOCK, lanes), BF16),
            pltpu.VMEM((8, PIECE, lanes), BF16),
            pltpu.VMEM((8, PIECE, lanes), BF16),
        ]
        + [dma((CHUNKS,))] * 6
        + [dma((3,))] * 2
        + [dma((3, CHUNKS))] * 2
        + [dma((2,))] * 2
        + [dma((2, 2))] * 4
        + [dma((2,))] * 2
        + [dma((8,))] * 2,
        compiler_params=pltpu.CompilerParams(collective_id=0, has_side_effects=True),
    )(
        jnp.swapaxes(saved_inputs[0], 1, 2),
        timesteps,
        time_table.T,
        skip_weight[0],
        ff_in[0].T,
        ff_out[0].T,
        jnp.swapaxes(output_cotangent, 1, 2),
    )
    grads, d_in, d_out, d_skip = pl.pallas_call(
        finish,
        out_shape=shapes,
        in_specs=[pl.BlockSpec(memory_space=pltpu.VMEM)] * 4,
        out_specs=(pl.BlockSpec(memory_space=pl.ANY),) * 4,
        scratch_shapes=[dma((4,))],
        compiler_params=pltpu.CompilerParams(vmem_limit_bytes=2**20),
    )(*held)
    grads = jnp.swapaxes(grads, 1, 2)[None]
    return (grads, d_skip, jnp.swapaxes(d_in, 0, 1), jnp.swapaxes(d_out, 0, 1))


def solution(mesh):
    split = Mesh(
        mesh.devices.reshape(mesh.shape["section"], 8, 4, 2, 2), ("section", "z", "x", "w", "core")
    )
    return jax.shard_map(
        shards,
        mesh=split,
        in_specs=(
            P("section", None, DP, None),
            P(None, DP),
            P(),
            P("section", None, None),
            P("section", None, None),
            P("section", None, None),
            P(None, DP, None),
        ),
        out_specs=(
            P("section", None, DP, None),
            P("section", DP),
            P("section", DP, None),
            P("section", DP, None),
        ),
        check_vma=False,
    )
```

```python
import jax
import jax.numpy as jnp
from jax import lax
from jax.experimental import pallas as pl
from jax.experimental.pallas import tpu as pltpu
from jax.sharding import Mesh
from jax.sharding import PartitionSpec as P

DP = ("z", "x", "w", "core")
MESH = pl.DeviceIdType.MESH
EPS = 1e-06
CHUNKS = 4
LAG = 3
FF_ROWS = 40
PIECE = 16
F32 = jnp.float32
BF16 = jnp.bfloat16


def dot(left, right):
    return jnp.dot(left, right, preferred_element_type=F32)


def dot_nt(left, right):
    return lax.dot_general(left, right, (((1,), (1,)), ((), ())), preferred_element_type=F32)


def kernel(
    xt_hbm,
    ts_hbm,
    tablet_hbm,
    wskip_hbm,
    wint_hbm,
    woutt_hbm,
    cott_hbm,
    grads_ref,
    din_ref,
    dout_ref,
    dskip_ref,
    xt_ref,
    ts_ref,
    tablet_ref,
    wskip_ref,
    wint_ref,
    woutt_ref,
    cott_ref,
    in_sem,
    ga_buf,
    v_msg,
    g_msg,
    k_msg,
    x_buf,
    z_buf,
    g_buf,
    vsend,
    csend,
    ksend,
    u_buf,
    r_buf,
    ds_buf,
    ch_buf,
    chsh_buf,
    nq,
    gq,
    sel,
    win_q,
    wout_q,
    win_n,
    wout_n,
    act_t,
    ds_q,
    gpre_t,
    za_t,
    zb_t,
    skip_part,
    skip_core,
    part,
    r_x1,
    r_x2,
    own_skip,
    r_own,
    z_send,
    r_z,
    vs_sem,
    vr_sem,
    cs_sem,
    cr_sem,
    ks_sem,
    kr_sem,
    n_s,
    n_r,
    gs_s,
    gs_r,
    gw_r,
    sk_s,
    sk_r,
    x1_s,
    x1_r,
    own_s,
    own_r,
    x2_s,
    x2_r,
    z_s,
    z_r,
):
    section = lax.axis_index("section")
    mz = lax.axis_index("z")
    mx = lax.axis_index("x")
    mw = lax.axis_index("w")
    mc = lax.axis_index("core")
    pairs = (
        (ts_hbm, ts_ref),
        (tablet_hbm, tablet_ref),
        (xt_hbm, xt_ref),
        (wskip_hbm, wskip_ref),
        (wint_hbm, wint_ref),
        (woutt_hbm, woutt_ref),
        (cott_hbm, cott_ref),
    )
    loads = [pltpu.make_async_copy(a, b, in_sem.at[i]) for i, (a, b) in enumerate(pairs)]
    for load in loads:
        load.start()
    micro, width, per = xt_ref.shape
    total = micro * per
    rows = total // CHUNKS
    levels = tablet_ref.shape[1]
    hidden = wint_ref.shape[1]

    def remote(src, dst, send, recv, device):
        return pltpu.make_async_remote_copy(
            src_ref=src,
            dst_ref=dst,
            send_sem=send,
            recv_sem=recv,
            device_id=device,
            device_id_type=MESH,
        )

    x_near = mx + 1 - 2 * lax.rem(mx, 2)
    x_far = 3 - mx
    x_op = lax.rem(mx + 2, 4)

    barrier = pltpu.get_barrier_semaphore()
    greet = [{"section": lax.rem(section + step, 4)} for step in (1, 3)]
    greet += [{"core": 1 - mc}, {"x": x_near}, {"x": x_far}, {"x": x_op}, {"w": 1 - mw}]
    greet += [{"w": 1 - mw, "x": to} for to in (x_near, x_far, x_op)]
    greet += [{"z": lax.rem(mz + step, 8)} for step in range(1, 8)]
    for device in greet:
        pl.semaphore_signal(barrier, inc=1, device_id=device, device_id_type=MESH)

    def at(c):
        if isinstance(c, int):
            return slice(c * rows, (c + 1) * rows)
        return pl.ds(pl.multiple_of(c * rows, rows), rows)

    def value_copy(c):
        device = {"section": 3 - section}
        return remote(vsend.at[c], v_msg.at[c], vs_sem.at[c], vr_sem.at[c], device)

    def chain_copy(c):
        device = {"section": lax.rem(section + 3, 4)}
        return remote(csend.at[c], g_msg.at[c], cs_sem.at[c], cr_sem.at[c], device)

    def skip_copy(c):
        device = {"section": lax.rem(section + 1, 4)}
        return remote(ksend.at[c], k_msg.at[c], ks_sem.at[c], kr_sem.at[c], device)

    def paced(copy, c):
        @pl.when(c >= 2)
        def _():
            copy(c - 2).wait_send()

        copy(c).start()

    rest = width - 256
    short = rows // 2

    def pack(buf, c, value):
        value = value.astype(BF16)
        buf[c, 0:rows, :] = value[:, 0:128]
        buf[c, rows : 2 * rows, :] = value[:, 128:256]
        buf[c, 2 * rows :, 0:rest] = value[0:short, 256:width]
        buf[c, 2 * rows :, rest:] = value[short:, 256:width]

    def unpack(buf, c):
        tail = jnp.concatenate([buf[c, 2 * rows :, 0:rest], buf[c, 2 * rows :, rest:]], axis=0)
        return jnp.concatenate([buf[c, 0:rows, :], buf[c, rows : 2 * rows, :], tail], axis=1)

    def front(c, z):
        united = x_buf[at(c), :] + dot(z, wskip_ref[...])
        recip = lax.rsqrt(jnp.mean(united * united, axis=-1, keepdims=True) + EPS)
        normed = (united * recip).astype(BF16)
        preact = dot(normed, wint_ref[...])
        sigma = jax.nn.sigmoid(preact)
        return united, recip, normed, preact, sigma, sigma * (1.0 + preact * (1.0 - sigma))

    def keep(c, united, recip, normed, slope):
        here = at(c)
        u_buf[here, :] = united
        r_buf[here, :] = jnp.broadcast_to(recip, (rows, 128))
        nq[me, here, 0:width] = normed
        ds_buf[here, :] = slope

    def encode(c):
        united, recip, normed, preact, sigma, slope = front(c, z_buf[at(c), :])
        active = (preact * sigma).astype(BF16)
        pack(vsend, c, united + dot(active, wout_n[...]))
        paced(value_copy, c)
        keep(c, united, recip, normed, slope)

    def back(gy, gact, united, recip, slope):
        pre = (gact * slope).astype(BF16)
        gn = dot(pre, win_n[...])
        mean = jnp.mean(gn * united, axis=-1, keepdims=True)
        chain = gy + recip * gn - united * (recip * recip * recip * mean)
        return chain.astype(BF16)

    def keep_chain(c, chain):
        here = at(c)
        ch_buf[here, 0:width] = chain
        chsh_buf[here, 64 : 64 + width] = chain

    def backward(c, which):
        here = at(c)
        chain_copy(c).wait_recv()
        if which == 1:

            @pl.when(c >= 2)
            def _():
                chain_copy(c - 2).wait_send()

        gy = unpack(g_msg, c).astype(F32)
        if which == 0:
            skip_copy(c).wait_recv()
            gy = gy + unpack(k_msg, c).astype(F32)
        low = gy.astype(BF16)
        gq[me, here, 64 : 64 + width] = low
        if which == 0:
            share(c)
        gact = dot(low, woutt_ref[...])
        chain = back(gy, gact, u_buf[here, :], r_buf[here, 0:1], ds_buf[here, :])
        if which == 1:
            pack(csend, c, chain)
            chain_copy(c).start()
        keep_chain(c, chain)

    def when(condition, action):
        pl.when(condition)(action)

    def step2_front(f):
        value_copy(f).wait_recv()
        z = unpack(v_msg, f)
        united, recip, normed, _, _, slope = front(f, z)
        z_buf[at(f), :] = z
        keep(f, united, recip, normed, slope)

    def step2_back(b):
        chain_copy(b).wait_recv()
        when(b >= 2, lambda: chain_copy(b - 2).wait_send())
        here = at(b)
        low = unpack(g_msg, b)
        gact = dot(low, woutt_ref[...])
        chain = back(low.astype(F32), gact, u_buf[here, :], r_buf[here, 0:1], ds_buf[here, :])
        joint = chain.astype(F32) + dot_nt(chain, wskip_ref[...]).astype(BF16).astype(F32)
        pack(csend, b, joint)
        chain_copy(b).start()
        gq[me, here, 64 : 64 + width] = low
        keep_chain(b, chain)

    def step3(c):
        here = at(c)
        value_copy(c).wait_recv()
        when(c >= 2, lambda: chain_copy(c - 2).wait_send())
        when(c >= 2, lambda: skip_copy(c - 2).wait_send())
        z = unpack(v_msg, c)
        united, recip, normed, _, _, slope = front(c, z)
        chain = back(g_buf[here, :].astype(F32), ga_buf[here, :], united, recip, slope)
        pack(csend, c, chain)
        chain_copy(c).start()
        pack(ksend, c, dot_nt(chain, wskip_ref[...]))
        skip_copy(c).start()
        z_buf[here, :] = z
        nq[me, here, 0:width] = normed
        keep_chain(c, chain)

    me = 2 * mw + mc
    mates = (2 * mw + 1 - mc, 2 * (1 - mw) + mc, 2 * (1 - mw) + 1 - mc)
    towards = ({"core": 1 - mc}, {"w": 1 - mw}, {"core": 1 - mc})

    def share_n(to):
        slot = mates[1] if to == 2 else me
        return remote(nq.at[slot], nq.at[slot], n_s.at[to], n_r.at[to], towards[to])

    def share_g(c, to):
        slot = mates[1] if to == 2 else me
        block = gq.at[slot, at(c)]
        got = gw_r.at[c] if to == 1 else gs_r.at[to]
        return remote(block, block, gs_s.at[to], got, towards[to])

    def whole_g(to):
        block = gq.at[me if to < 2 else mates[1]]
        return remote(block, block, gs_s.at[to], gs_r.at[to], towards[to])

    def share(c):
        for to in range(2):
            share_g(c, to).start()

    def share_normed():
        for to in range(2):
            share_n(to).start()

    nq[me, :, width:] = jnp.zeros((total, 384 - width), BF16)
    gq[me, :, 0:64] = jnp.zeros((total, 64), BF16)
    ch_buf[:, width:] = jnp.zeros((total, 384 - width), BF16)
    chsh_buf[:, 0:64] = jnp.zeros((total, 64), BF16)

    def rows_of(m):
        return slice(m * per, (m + 1) * per)

    def choose_units():
        line = lax.broadcasted_iota(jnp.int32, (hidden, width), 1)
        unit = 40 * (4 * (lax.rem(line, 80) // 10) + line // 80) + 10 * me + lax.rem(line, 10)
        chosen = lax.broadcasted_iota(jnp.int32, (hidden, width), 0) == unit
        sel[...] = jnp.where(chosen, 1.0, 0.0).astype(BF16)
        win_q[...] = dot(wint_ref[...], sel[...]).astype(BF16)
        wout_q[0:64, :] = jnp.zeros((64, width), BF16)
        wout_q[64:, :] = dot(woutt_ref[...], sel[...]).astype(BF16)

    def embed(m):
        onehot = ts_ref[m : m + 1, :] == lax.broadcasted_iota(jnp.int32, (levels, per), 0)
        rows_t = dot(tablet_ref[...], jnp.where(onehot, 1.0, 0.0).astype(BF16))
        z_buf[rows_of(m), :] = rows_t.T.astype(BF16)

    for load in loads[0:3]:
        load.wait()

    @pl.when(section < 2)
    def _():
        for m in range(micro):
            embed(m)

    for m in range(micro):
        x_buf[rows_of(m), :] = xt_ref[m].astype(F32).T
    for load in loads[3:]:
        load.wait()

    @pl.when(section == 3)
    def _():
        for m in range(micro):
            cot = cott_ref[m].astype(F32).T.astype(BF16)
            g_buf[rows_of(m), :] = cot
            gq[me, rows_of(m), 64 : 64 + width] = cot
        ga_buf[...] = dot(g_buf[...], woutt_ref[...])

    @pl.when(section < 2)
    def _():
        wout_n[...] = woutt_ref[...].T

    @pl.when(section >= 2)
    def _():
        win_n[...] = wint_ref[...].T

    pl.semaphore_wait(barrier, len(greet))

    @pl.when(section < 2)
    def _():
        @pl.loop(0, CHUNKS)
        def _(c):
            encode(c)

        share_normed()
        win_n[...] = wint_ref[...].T
        choose_units()

    @pl.when(section == 3)
    def _():
        @pl.loop(0, CHUNKS)
        def _(c):
            share(c)

        choose_units()

        @pl.loop(0, CHUNKS)
        def _(c):
            step3(c)

        share_normed()

    @pl.when(section == 2)
    def _():
        choose_units()

        @pl.loop(0, LAG)
        def _(t):
            step2_front(t)

        @pl.loop(0, CHUNKS)
        def _(t):
            step2_back(t)

            @pl.when(t < CHUNKS - LAG)
            def _():
                step2_front(t + LAG)

        share_normed()

    slot = lax.broadcasted_iota(jnp.int32, (256, width), 0)
    channel = lax.broadcasted_iota(jnp.int32, (256, width), 1)
    third = lax.rem(slot, 2)
    pixel = lax.rem(slot, 64) // 2
    first = 10 * (4 * lax.rem(pixel, 8) + pixel // 8) + 5 * lax.rem(slot // 64, 2)
    first = first + 2 * (slot // 128)
    for dst, pick in (
        (za_t, channel == first + 2 * third),
        (zb_t, (channel == first + 1) & (third == 0)),
    ):
        dst[...] = dot_nt(jnp.where(pick, 1.0, 0.0).astype(BF16), z_buf[...]).astype(BF16)

    share_n(1).wait_recv()
    share_n(2).start()
    share_n(0).wait_recv()
    share_n(2).wait_recv()

    @pl.loop(0, 4)
    def _(q):
        preact = dot(nq[q, :, 0:width], win_q[...])
        sigma = jax.nn.sigmoid(preact)
        ds_q[q] = sigma * (1.0 + preact * (1.0 - sigma))
        act_t[:, pl.ds(pl.multiple_of(q * total, total), total)] = (preact * sigma).astype(BF16).T

    for which in (0, 1):

        @pl.when(section == which)
        def _():
            @pl.loop(0, CHUNKS)
            def _(c):
                backward(c, which)

    def joined(left, right):
        return left[:, 0:256], left[:, 256:384] + right[:, 0:128], right[:, 128:384]

    edges = (slice(0, 256), slice(256, 384), slice(384, 640))

    @pl.when((section == 1) | (section == 2))
    def _():
        @pl.loop(0, CHUNKS)
        def _(c):
            share(c)

    skips = joined(dot(za_t[...], ch_buf[...]), dot(zb_t[...], chsh_buf[...]))
    for edge, value in zip(edges, skips):
        skip_part[:, :, :, edge] = value.astype(BF16).reshape(2, 2, 64, -1)
    skip1 = remote(skip_part.at[1 - mc], skip_core, sk_s.at[0], sk_r.at[0], {"core": 1 - mc})
    skip1.start()

    def own_copy(k):
        v = 1 - mw if k % 2 else mw
        to = (mx, x_near, x_far, x_op)[k // 2]
        return remote(own_skip.at[v, to], r_own.at[k - 1], own_s.at[0], own_r.at[0], {"w": v, "x": to})


    @pl.loop(0, CHUNKS)
    def _(c):
        share_g(c, 1).wait_recv()
        share_g(c, 2).start()

    skip1.wait_recv()
    for v in range(2):
        mine = skip_part[mc, v].astype(F32) + skip_core[v].astype(F32)
        own_skip[v] = mine.astype(BF16).reshape(4, PIECE, 2 * width)
    def through(q):
        pre = (dot(gq[q], wout_q[...]) * ds_q[q]).astype(BF16)
        gpre_t[:, pl.ds(pl.multiple_of(q * total, total), total)] = pre.T

    through(me)
    through(mates[1])
    for to in (0, 2):
        whole_g(to).wait_recv()
        through(mates[to])

    everyone = 4 * total
    d_out = dot(act_t[...], gq[...].reshape(everyone, 384))
    d_in = dot(gpre_t[...], nq[...].reshape(everyone, 384))
    for edge, value in zip(edges, joined(d_in, d_out)):
        value = value.astype(BF16).reshape(4, 2, FF_ROWS, -1)
        for color in range(2):
            part[color, :, :, edge] = value[:, color]

    def x1_copy(color, k):
        device = x_far if color else x_near
        block = device if k == 0 else x_op
        src, dst = part.at[color, block], r_x1.at[color, k]
        return remote(src, dst, x1_s.at[color, k], x1_r.at[color, k], {"x": device})

    def x2_copy(color):
        device = x_near if color else x_far
        src = part.at[color, device]
        return remote(src, r_x2.at[color], x2_s.at[color], x2_r.at[color], {"x": device})

    for k in (1, 0):
        for color in range(2):
            x1_copy(color, k).start()
    for k in range(7, 0, -1):
        own_copy(k).start()
    for m in range(micro):
        grads_ref[m] = ch_buf[m * per : (m + 1) * per, 0:width].astype(F32).T.astype(BF16)

    def added(left, right):
        return left.astype(F32) + right.astype(F32)

    for k in (1, 0):
        for color in range(2):
            x1_copy(color, k).wait_recv()
            block = mx if k == 0 else (x_near if color else x_far)
            part[color, block] = added(part[color, block], r_x1[color, k]).astype(BF16)
            if k == 1:
                x2_copy(color).start()

    def z_copy(k):
        target = lax.rem(mz + k, 8)
        return remote(z_send.at[target], r_z.at[k - 1], z_s.at[0], z_r.at[0], {"z": target})

    for to in range(3):
        share_n(to).wait_send()
    skip1.wait_send()

    for to in range(3):
        whole_g(to).wait_send()

    @pl.when(section < 2)
    def _():
        for late in range(1, 3):
            value_copy(CHUNKS - late).wait_send()

    @pl.when(section > 0)
    def _():
        for late in range(1, 3):
            chain_copy(CHUNKS - late).wait_send()

    @pl.when(section == 3)
    def _():
        for late in range(1, 3):
            skip_copy(CHUNKS - late).wait_send()

    tails = own_skip[mw, mx].astype(F32)
    all_own = remote(r_own, r_own, own_s.at[0], own_r.at[0], {"w": 1 - mw})
    all_own.wait_recv()
    for k in range(7):
        tails = tails + r_own[k].astype(F32)
    for color in range(2):
        x2_copy(color).wait_recv()
        block = added(part[color, mx], r_x2[color])
        for j in range(4):
            piece = (block[10 * j : 10 * j + 10], tails[8 * color + 2 * j : 8 * color + 2 * j + 2])
            piece = jnp.concatenate(piece, axis=0)
            stack = [piece[:, 128 * t : 128 * t + 128] for t in range(5)]
            stack = jnp.concatenate(stack + [jnp.zeros((4, 128), F32)], axis=0)
            z_send[4 * color + j] = stack.astype(BF16)
    far_first = (4, 3, 5, 2, 6, 1, 7)
    for k in far_first:
        z_copy(k).start()
    acc = z_send[mz].astype(F32)
    all_z = remote(r_z, r_z, z_s.at[0], z_r.at[0], {"z": lax.rem(mz + 1, 8)})
    all_z.wait_recv()
    for k in range(7):
        acc = acc + r_z[k].astype(F32)
    acc = jnp.concatenate([acc[12 * t : 12 * t + 12] for t in range(5)], axis=1)

    for j in range(10):
        din_ref[j] = acc[j : j + 1, 0:width]
        dout_ref[j] = acc[j : j + 1, width:]
    half = width // 2
    lead, mid, last = acc[10:11, 0:width], acc[10:11, width:], acc[11:12, 0:width]

    @pl.when(mc == 0)
    def _():
        dskip_ref[:, 0:width] = lead
        dskip_ref[:, width : 2 * width] = mid
        dskip_ref[:, 2 * width :] = last[:, 0:half]

    @pl.when(mc == 1)
    def _():
        dskip_ref[:, 0:half] = lead[:, half:]
        dskip_ref[:, half : half + width] = mid
        dskip_ref[:, half + width :] = last

    for color in range(2):
        for k in range(2):
            x1_copy(color, k).wait_send()
        x2_copy(color).wait_send()
    all_own.wait_send()
    all_z.wait_send()


def finish(*refs):
    copies = [pltpu.make_async_copy(refs[i], refs[4 + i], refs[8].at[i]) for i in range(4)]
    for copy in copies:
        copy.start()
    for copy in copies:
        copy.wait()


def shards(saved_inputs, timesteps, time_table, skip_weight, ff_in, ff_out, output_cotangent):
    n_micro, per, width = saved_inputs.shape[1:]
    hidden = ff_in.shape[1]
    total = n_micro * per
    lanes = 2 * width
    shapes = (
        jax.ShapeDtypeStruct((n_micro, width, per), BF16),
        jax.ShapeDtypeStruct((10, 1, width), F32),
        jax.ShapeDtypeStruct((10, 1, width), F32),
        jax.ShapeDtypeStruct((1, 800), F32),
    )
    low = pltpu.VMEM((total, width), BF16)
    message = pltpu.VMEM((CHUNKS, total // CHUNKS * width // 128, 128), BF16)
    wide = pltpu.VMEM((total, 384), BF16)
    dma = pltpu.SemaphoreType.DMA
    held = pl.pallas_call(
        kernel,
        out_shape=tuple(pltpu.VMEM(s.shape, s.dtype) for s in shapes),
        in_specs=[pl.BlockSpec(memory_space=pl.ANY)] * 7,
        out_specs=(pl.BlockSpec(memory_space=pltpu.VMEM),) * 4,
        scratch_shapes=[
            pltpu.VMEM((n_micro, width, per), BF16),
            pltpu.VMEM(timesteps.shape, jnp.int32),
            pltpu.VMEM((width, time_table.shape[0]), BF16),
            pltpu.VMEM((width, width), BF16),
            pltpu.VMEM((width, hidden), BF16),
            pltpu.VMEM((width, hidden), BF16),
            pltpu.VMEM((n_micro, width, per), BF16),
            dma((7,)),
            pltpu.VMEM((total, hidden), F32),
            message,
            message,
            message,
            pltpu.VMEM((total, width), F32),
            low,
            low,
            message,
            message,
            message,
            pltpu.VMEM((total, width), F32),
            pltpu.VMEM((total, 128), F32),
            pltpu.VMEM((total, hidden), F32),
            wide,
            wide,
            pltpu.VMEM((4, total, 384), BF16),
            pltpu.VMEM((4, total, 384), BF16),
            pltpu.VMEM((hidden, width), BF16),
            pltpu.VMEM((width, width), BF16),
            pltpu.VMEM((384, width), BF16),
            pltpu.VMEM((hidden, width), BF16),
            pltpu.VMEM((hidden, width), BF16),
            pltpu.VMEM((width, 4 * total), BF16),
            pltpu.VMEM((4, total, width), F32),
            pltpu.VMEM((width, 4 * total), BF16),
            pltpu.VMEM((256, total), BF16),
            pltpu.VMEM((256, total), BF16),
            pltpu.VMEM((2, 2, 64, lanes), BF16),
            pltpu.VMEM((2, 64, lanes), BF16),
            pltpu.VMEM((2, 4, FF_ROWS, lanes), BF16),
            pltpu.VMEM((2, 2, FF_ROWS, lanes), BF16),
            pltpu.VMEM((2, FF_ROWS, lanes), BF16),
            pltpu.VMEM((2, 4, PIECE, lanes), BF16),
            pltpu.VMEM((7, PIECE, lanes), BF16),
            pltpu.VMEM((8, 64, 128), BF16),
            pltpu.VMEM((7, 64, 128), BF16),
        ]
        + [dma((CHUNKS,))] * 6
        + [dma((3,))] * 2
        + [dma((3,))] * 2
        + [dma((CHUNKS,))]
        + [dma((1,))] * 2
        + [dma((2, 2))] * 2
        + [dma((1,))] * 2
        + [dma((2,))] * 2
        + [dma((1,))] * 2,
        compiler_params=pltpu.CompilerParams(collective_id=0, has_side_effects=True),
    )(
        jnp.swapaxes(saved_inputs[0], 1, 2),
        timesteps,
        time_table.T,
        skip_weight[0],
        ff_in[0].T,
        ff_out[0].T,
        jnp.swapaxes(output_cotangent, 1, 2),
    )
    grads, d_in, d_out, d_skip = pl.pallas_call(
        finish,
        out_shape=shapes,
        in_specs=[pl.BlockSpec(memory_space=pltpu.VMEM)] * 4,
        out_specs=(pl.BlockSpec(memory_space=pl.ANY),) * 4,
        scratch_shapes=[dma((4,))],
        compiler_params=pltpu.CompilerParams(vmem_limit_bytes=2**20),
    )(*held)
    grads = jnp.swapaxes(grads, 1, 2)[None]
    return (grads, d_skip, jnp.swapaxes(d_in, 0, 1), jnp.swapaxes(d_out, 0, 1))


def solution(mesh):
    split = Mesh(
        mesh.devices.reshape(mesh.shape["section"], 8, 4, 2, 2), ("section", "z", "x", "w", "core")
    )
    return jax.shard_map(
        shards,
        mesh=split,
        in_specs=(
            P("section", None, DP, None),
            P(None, DP),
            P(),
            P("section", None, None),
            P("section", None, None),
            P("section", None, None),
            P(None, DP, None),
        ),
        out_specs=(
            P("section", None, DP, None),
            P("section", DP),
            P("section", DP, None),
            P("section", DP, None),
        ),
        check_vma=False,
    )
```

```python
import jax
import jax.numpy as jnp
from jax import lax
from jax.experimental import pallas as pl
from jax.experimental.pallas import tpu as pltpu
from jax.sharding import Mesh
from jax.sharding import PartitionSpec as P

DP = ("z", "x", "w", "core")
MESH = pl.DeviceIdType.MESH
EPS = 1e-06
CHUNKS = 8
LAG = 5
FF_ROWS = 40
PIECE = 16
F32 = jnp.float32
BF16 = jnp.bfloat16


def dot(left, right):
    return jnp.dot(left, right, preferred_element_type=F32)


def dot_nt(left, right):
    return lax.dot_general(left, right, (((1,), (1,)), ((), ())), preferred_element_type=F32)


def kernel(
    xt_hbm,
    ts_hbm,
    tablet_hbm,
    wskip_hbm,
    wint_hbm,
    woutt_hbm,
    cott_hbm,
    grads_ref,
    din_ref,
    dout_ref,
    dskip_ref,
    xt_ref,
    ts_ref,
    tablet_ref,
    wskip_ref,
    wint_ref,
    woutt_ref,
    cott_ref,
    in_sem,
    ga_buf,
    v_msg,
    g_msg,
    k_msg,
    x_buf,
    z_buf,
    g_buf,
    vsend,
    csend,
    ksend,
    u_buf,
    r_buf,
    ds_buf,
    ch_buf,
    chsh_buf,
    nq,
    gq,
    sel,
    win_q,
    wout_q,
    win_n,
    wout_n,
    act_t,
    ds_q,
    gpre_t,
    za_t,
    zb_t,
    skip_part,
    skip_core,
    part,
    r_x1,
    r_x2,
    own_skip,
    r_own,
    z_send,
    r_z,
    vs_sem,
    vr_sem,
    cs_sem,
    cr_sem,
    ks_sem,
    kr_sem,
    n_s,
    n_r,
    gs_s,
    gs_r,
    gw_r,
    sk_s,
    sk_r,
    x1_s,
    x1_r,
    own_s,
    own_r,
    x2_s,
    x2_r,
    z_s,
    z_r,
):
    section = lax.axis_index("section")
    mz = lax.axis_index("z")
    mx = lax.axis_index("x")
    mw = lax.axis_index("w")
    mc = lax.axis_index("core")
    pairs = (
        (ts_hbm, ts_ref),
        (tablet_hbm, tablet_ref),
        (xt_hbm, xt_ref),
        (wskip_hbm, wskip_ref),
        (wint_hbm, wint_ref),
        (woutt_hbm, woutt_ref),
        (cott_hbm, cott_ref),
    )
    loads = [pltpu.make_async_copy(a, b, in_sem.at[i]) for i, (a, b) in enumerate(pairs)]
    for load in loads:
        load.start()
    micro, width, per = xt_ref.shape
    total = micro * per
    rows = total // CHUNKS
    levels = tablet_ref.shape[1]
    hidden = wint_ref.shape[1]

    def remote(src, dst, send, recv, device):
        return pltpu.make_async_remote_copy(
            src_ref=src,
            dst_ref=dst,
            send_sem=send,
            recv_sem=recv,
            device_id=device,
            device_id_type=MESH,
        )

    x_near = mx + 1 - 2 * lax.rem(mx, 2)
    x_far = 3 - mx
    x_op = lax.rem(mx + 2, 4)

    barrier = pltpu.get_barrier_semaphore()
    greet = [{"section": lax.rem(section + step, 4)} for step in (1, 3)]
    greet += [{"core": 1 - mc}, {"x": x_near}, {"x": x_far}, {"x": x_op}, {"w": 1 - mw}]
    greet += [{"w": 1 - mw, "x": to} for to in (x_near, x_far, x_op)]
    greet += [{"z": lax.rem(mz + step, 8)} for step in range(1, 8)]
    for device in greet:
        pl.semaphore_signal(barrier, inc=1, device_id=device, device_id_type=MESH)

    def at(c):
        if isinstance(c, int):
            return slice(c * rows, (c + 1) * rows)
        return pl.ds(pl.multiple_of(c * rows, rows), rows)

    def value_copy(c):
        device = {"section": 3 - section}
        return remote(vsend.at[c], v_msg.at[c], vs_sem.at[c], vr_sem.at[c], device)

    def chain_copy(c):
        device = {"section": lax.rem(section + 3, 4)}
        return remote(csend.at[c], g_msg.at[c], cs_sem.at[c], cr_sem.at[c], device)

    def skip_copy(c):
        device = {"section": lax.rem(section + 1, 4)}
        return remote(ksend.at[c], k_msg.at[c], ks_sem.at[c], kr_sem.at[c], device)

    def paced(copy, c):
        @pl.when(c >= 2)
        def _():
            copy(c - 2).wait_send()

        copy(c).start()

    rest = width - 256
    short = rows // 2

    def pack(buf, c, value):
        value = value.astype(BF16)
        buf[c, 0:rows, :] = value[:, 0:128]
        buf[c, rows : 2 * rows, :] = value[:, 128:256]
        buf[c, 2 * rows :, 0:rest] = value[0:short, 256:width]
        buf[c, 2 * rows :, rest:] = value[short:, 256:width]

    def unpack(buf, c):
        tail = jnp.concatenate([buf[c, 2 * rows :, 0:rest], buf[c, 2 * rows :, rest:]], axis=0)
        return jnp.concatenate([buf[c, 0:rows, :], buf[c, rows : 2 * rows, :], tail], axis=1)

    def front(c, z):
        united = x_buf[at(c), :] + dot(z, wskip_ref[...])
        recip = lax.rsqrt(jnp.mean(united * united, axis=-1, keepdims=True) + EPS)
        normed = (united * recip).astype(BF16)
        preact = dot(normed, wint_ref[...])
        sigma = jax.nn.sigmoid(preact)
        return united, recip, normed, preact, sigma, sigma * (1.0 + preact * (1.0 - sigma))

    def keep(c, united, recip, normed, slope):
        here = at(c)
        u_buf[here, :] = united
        r_buf[here, :] = jnp.broadcast_to(recip, (rows, 128))
        nq[me, here, 0:width] = normed
        ds_buf[here, :] = slope

    def encode(c):
        united, recip, normed, preact, sigma, slope = front(c, z_buf[at(c), :])
        active = (preact * sigma).astype(BF16)
        pack(vsend, c, united + dot(active, wout_n[...]))
        paced(value_copy, c)
        keep(c, united, recip, normed, slope)

    def back(gy, gact, united, recip, slope):
        pre = (gact * slope).astype(BF16)
        gn = dot(pre, win_n[...])
        mean = jnp.mean(gn * united, axis=-1, keepdims=True)
        chain = gy + recip * gn - united * (recip * recip * recip * mean)
        return chain.astype(BF16)

    def keep_chain(c, chain):
        here = at(c)
        ch_buf[here, 0:width] = chain
        chsh_buf[here, 64 : 64 + width] = chain

    def backward(c, which):
        here = at(c)
        chain_copy(c).wait_recv()
        if which == 1:

            @pl.when(c >= 3)
            def _():
                chain_copy(c - 3).wait_send()

        gy = unpack(g_msg, c).astype(F32)
        if which == 0:
            skip_copy(c).wait_recv()
            gy = gy + unpack(k_msg, c).astype(F32)
        low = gy.astype(BF16)
        gq[me, here, 64 : 64 + width] = low
        if which == 0:
            share(c)
        gact = dot(low, woutt_ref[...])
        chain = back(gy, gact, u_buf[here, :], r_buf[here, 0:1], ds_buf[here, :])
        if which == 1:
            pack(csend, c, chain)
            chain_copy(c).start()
        keep_chain(c, chain)

    def when(condition, action):
        pl.when(condition)(action)

    def step2_front(f):
        value_copy(f).wait_recv()
        z = unpack(v_msg, f)
        united, recip, normed, _, _, slope = front(f, z)
        z_buf[at(f), :] = z
        keep(f, united, recip, normed, slope)

    def step2_back(b):
        chain_copy(b).wait_recv()
        when(b >= 3, lambda: chain_copy(b - 3).wait_send())
        here = at(b)
        low = unpack(g_msg, b)
        gact = dot(low, woutt_ref[...])
        chain = back(low.astype(F32), gact, u_buf[here, :], r_buf[here, 0:1], ds_buf[here, :])
        joint = chain.astype(F32) + dot_nt(chain, wskip_ref[...]).astype(BF16).astype(F32)
        pack(csend, b, joint)
        chain_copy(b).start()
        gq[me, here, 64 : 64 + width] = low
        keep_chain(b, chain)

    def step3(c):
        here = at(c)
        value_copy(c).wait_recv()
        when(c >= 3, lambda: chain_copy(c - 3).wait_send())
        when(c >= 2, lambda: skip_copy(c - 2).wait_send())
        z = unpack(v_msg, c)
        united, recip, normed, _, _, slope = front(c, z)
        chain = back(g_buf[here, :].astype(F32), ga_buf[here, :], united, recip, slope)
        pack(csend, c, chain)
        chain_copy(c).start()
        pack(ksend, c, dot_nt(chain, wskip_ref[...]))
        skip_copy(c).start()
        z_buf[here, :] = z
        nq[me, here, 0:width] = normed
        keep_chain(c, chain)

    me = 2 * mw + mc
    mates = (2 * mw + 1 - mc, 2 * (1 - mw) + mc, 2 * (1 - mw) + 1 - mc)
    towards = ({"core": 1 - mc}, {"w": 1 - mw}, {"core": 1 - mc})

    def share_n(to):
        slot = mates[1] if to == 2 else me
        return remote(nq.at[slot], nq.at[slot], n_s.at[to], n_r.at[to], towards[to])

    def share_g(c, to):
        slot = mates[1] if to == 2 else me
        block = gq.at[slot, at(c)]
        got = gw_r.at[c] if to == 1 else gs_r.at[to]
        return remote(block, block, gs_s.at[to], got, towards[to])

    def whole_g(to):
        block = gq.at[me if to < 2 else mates[1]]
        return remote(block, block, gs_s.at[to], gs_r.at[to], towards[to])

    def share(c):
        for to in range(2):
            share_g(c, to).start()

    def share_normed():
        for to in range(2):
            share_n(to).start()

    nq[me, :, width:] = jnp.zeros((total, 384 - width), BF16)
    gq[me, :, 0:64] = jnp.zeros((total, 64), BF16)
    ch_buf[:, width:] = jnp.zeros((total, 384 - width), BF16)
    chsh_buf[:, 0:64] = jnp.zeros((total, 64), BF16)

    def rows_of(m):
        return slice(m * per, (m + 1) * per)

    def choose_units():
        line = lax.broadcasted_iota(jnp.int32, (hidden, width), 1)
        unit = 40 * (4 * (lax.rem(line, 80) // 10) + line // 80) + 10 * me + lax.rem(line, 10)
        chosen = lax.broadcasted_iota(jnp.int32, (hidden, width), 0) == unit
        sel[...] = jnp.where(chosen, 1.0, 0.0).astype(BF16)
        win_q[...] = dot(wint_ref[...], sel[...]).astype(BF16)
        wout_q[0:64, :] = jnp.zeros((64, width), BF16)
        wout_q[64:, :] = dot(woutt_ref[...], sel[...]).astype(BF16)

    def embed(m):
        onehot = ts_ref[m : m + 1, :] == lax.broadcasted_iota(jnp.int32, (levels, per), 0)
        rows_t = dot(tablet_ref[...], jnp.where(onehot, 1.0, 0.0).astype(BF16))
        z_buf[rows_of(m), :] = rows_t.T.astype(BF16)

    for load in loads[0:3]:
        load.wait()

    @pl.when(section < 2)
    def _():
        for m in range(micro):
            embed(m)

    for m in range(micro):
        x_buf[rows_of(m), :] = xt_ref[m].astype(F32).T
    for load in loads[3:]:
        load.wait()

    @pl.when(section == 3)
    def _():
        for m in range(micro):
            cot = cott_ref[m].astype(F32).T.astype(BF16)
            g_buf[rows_of(m), :] = cot
            gq[me, rows_of(m), 64 : 64 + width] = cot
        ga_buf[...] = dot(g_buf[...], woutt_ref[...])

    @pl.when(section < 2)
    def _():
        wout_n[...] = woutt_ref[...].T

    @pl.when(section >= 2)
    def _():
        win_n[...] = wint_ref[...].T

    pl.semaphore_wait(barrier, len(greet))

    @pl.when(section < 2)
    def _():
        @pl.loop(0, CHUNKS)
        def _(c):
            encode(c)

        share_normed()
        win_n[...] = wint_ref[...].T
        choose_units()

    @pl.when(section == 3)
    def _():
        @pl.loop(0, CHUNKS)
        def _(c):
            share(c)

        choose_units()

        @pl.loop(0, CHUNKS)
        def _(c):
            step3(c)

        share_normed()

    @pl.when(section == 2)
    def _():
        choose_units()

        @pl.loop(0, LAG)
        def _(t):
            step2_front(t)

        @pl.loop(0, CHUNKS)
        def _(t):
            step2_back(t)

            @pl.when(t < CHUNKS - LAG)
            def _():
                step2_front(t + LAG)

        share_normed()

    slot = lax.broadcasted_iota(jnp.int32, (256, width), 0)
    channel = lax.broadcasted_iota(jnp.int32, (256, width), 1)
    third = lax.rem(slot, 2)
    pixel = lax.rem(slot, 64) // 2
    first = 10 * (4 * lax.rem(pixel, 8) + pixel // 8) + 5 * lax.rem(slot // 64, 2)
    first = first + 2 * (slot // 128)
    for dst, pick in (
        (za_t, channel == first + 2 * third),
        (zb_t, (channel == first + 1) & (third == 0)),
    ):
        dst[...] = dot_nt(jnp.where(pick, 1.0, 0.0).astype(BF16), z_buf[...]).astype(BF16)

    share_n(1).wait_recv()
    share_n(2).start()
    share_n(0).wait_recv()
    share_n(2).wait_recv()

    @pl.loop(0, 4)
    def _(q):
        preact = dot(nq[q, :, 0:width], win_q[...])
        sigma = jax.nn.sigmoid(preact)
        ds_q[q] = sigma * (1.0 + preact * (1.0 - sigma))
        act_t[:, pl.ds(pl.multiple_of(q * total, total), total)] = (preact * sigma).astype(BF16).T

    for which in (0, 1):

        @pl.when(section == which)
        def _():
            @pl.loop(0, CHUNKS)
            def _(c):
                backward(c, which)

    def joined(left, right):
        return left[:, 0:256], left[:, 256:384] + right[:, 0:128], right[:, 128:384]

    edges = (slice(0, 256), slice(256, 384), slice(384, 640))

    @pl.when((section == 1) | (section == 2))
    def _():
        @pl.loop(0, CHUNKS)
        def _(c):
            share(c)

    skips = joined(dot(za_t[...], ch_buf[...]), dot(zb_t[...], chsh_buf[...]))
    for edge, value in zip(edges, skips):
        skip_part[:, :, :, edge] = value.astype(BF16).reshape(2, 2, 64, -1)
    skip1 = remote(skip_part.at[1 - mc], skip_core, sk_s.at[0], sk_r.at[0], {"core": 1 - mc})
    skip1.start()

    def own_copy(k):
        v = 1 - mw if k % 2 else mw
        to = (mx, x_near, x_far, x_op)[k // 2]
        return remote(own_skip.at[v, to], r_own.at[k - 1], own_s.at[0], own_r.at[0], {"w": v, "x": to})


    @pl.loop(0, CHUNKS)
    def _(c):
        share_g(c, 1).wait_recv()
        share_g(c, 2).start()

    skip1.wait_recv()
    for v in range(2):
        mine = skip_part[mc, v].astype(F32) + skip_core[v].astype(F32)
        own_skip[v] = mine.astype(BF16).reshape(4, PIECE, 2 * width)
    def through(q):
        pre = (dot(gq[q], wout_q[...]) * ds_q[q]).astype(BF16)
        gpre_t[:, pl.ds(pl.multiple_of(q * total, total), total)] = pre.T

    through(me)
    through(mates[1])
    for to in (0, 2):
        whole_g(to).wait_recv()
        through(mates[to])

    everyone = 4 * total
    d_out = dot(act_t[...], gq[...].reshape(everyone, 384))
    d_in = dot(gpre_t[...], nq[...].reshape(everyone, 384))
    for edge, value in zip(edges, joined(d_in, d_out)):
        value = value.astype(BF16).reshape(4, 2, FF_ROWS, -1)
        for color in range(2):
            part[color, :, :, edge] = value[:, color]

    def x1_copy(color, k):
        device = x_far if color else x_near
        block = device if k == 0 else x_op
        src, dst = part.at[color, block], r_x1.at[color, k]
        return remote(src, dst, x1_s.at[color, k], x1_r.at[color, k], {"x": device})

    def x2_copy(color):
        device = x_near if color else x_far
        src = part.at[color, device]
        return remote(src, r_x2.at[color], x2_s.at[color], x2_r.at[color], {"x": device})

    for k in (1, 0):
        for color in range(2):
            x1_copy(color, k).start()
    for k in range(7, 0, -1):
        own_copy(k).start()
    for m in range(micro):
        grads_ref[m] = ch_buf[m * per : (m + 1) * per, 0:width].astype(F32).T.astype(BF16)

    def added(left, right):
        return left.astype(F32) + right.astype(F32)

    for k in (1, 0):
        for color in range(2):
            x1_copy(color, k).wait_recv()
            block = mx if k == 0 else (x_near if color else x_far)
            part[color, block] = added(part[color, block], r_x1[color, k]).astype(BF16)
            if k == 1:
                x2_copy(color).start()

    def z_copy(k):
        target = lax.rem(mz + k, 8)
        return remote(z_send.at[target], r_z.at[k - 1], z_s.at[0], z_r.at[0], {"z": target})

    for to in range(3):
        share_n(to).wait_send()
    skip1.wait_send()

    for to in range(3):
        whole_g(to).wait_send()

    @pl.when(section < 2)
    def _():
        for late in range(1, 3):
            value_copy(CHUNKS - late).wait_send()

    @pl.when(section > 0)
    def _():
        for late in range(1, 4):
            chain_copy(CHUNKS - late).wait_send()

    @pl.when(section == 3)
    def _():
        for late in range(1, 3):
            skip_copy(CHUNKS - late).wait_send()

    tails = own_skip[mw, mx].astype(F32)
    all_own = remote(r_own, r_own, own_s.at[0], own_r.at[0], {"w": 1 - mw})
    all_own.wait_recv()
    for k in range(7):
        tails = tails + r_own[k].astype(F32)
    for color in range(2):
        x2_copy(color).wait_recv()
        block = added(part[color, mx], r_x2[color])
        for j in range(4):
            piece = (block[10 * j : 10 * j + 10], tails[8 * color + 2 * j : 8 * color + 2 * j + 2])
            piece = jnp.concatenate(piece, axis=0)
            stack = [piece[:, 128 * t : 128 * t + 128] for t in range(5)]
            stack = jnp.concatenate(stack + [jnp.zeros((4, 128), F32)], axis=0)
            z_send[4 * color + j] = stack.astype(BF16)
    far_first = (4, 3, 5, 2, 6, 1, 7)
    for k in far_first:
        z_copy(k).start()
    acc = z_send[mz].astype(F32)
    all_z = remote(r_z, r_z, z_s.at[0], z_r.at[0], {"z": lax.rem(mz + 1, 8)})
    all_z.wait_recv()
    for k in range(7):
        acc = acc + r_z[k].astype(F32)
    acc = jnp.concatenate([acc[12 * t : 12 * t + 12] for t in range(5)], axis=1)

    for j in range(10):
        din_ref[j] = acc[j : j + 1, 0:width]
        dout_ref[j] = acc[j : j + 1, width:]
    half = width // 2
    lead, mid, last = acc[10:11, 0:width], acc[10:11, width:], acc[11:12, 0:width]

    @pl.when(mc == 0)
    def _():
        dskip_ref[:, 0:width] = lead
        dskip_ref[:, width : 2 * width] = mid
        dskip_ref[:, 2 * width :] = last[:, 0:half]

    @pl.when(mc == 1)
    def _():
        dskip_ref[:, 0:half] = lead[:, half:]
        dskip_ref[:, half : half + width] = mid
        dskip_ref[:, half + width :] = last

    for color in range(2):
        for k in range(2):
            x1_copy(color, k).wait_send()
        x2_copy(color).wait_send()
    all_own.wait_send()
    all_z.wait_send()


def finish(*refs):
    copies = [pltpu.make_async_copy(refs[i], refs[4 + i], refs[8].at[i]) for i in range(4)]
    for copy in copies:
        copy.start()
    for copy in copies:
        copy.wait()


def shards(saved_inputs, timesteps, time_table, skip_weight, ff_in, ff_out, output_cotangent):
    n_micro, per, width = saved_inputs.shape[1:]
    hidden = ff_in.shape[1]
    total = n_micro * per
    lanes = 2 * width
    shapes = (
        jax.ShapeDtypeStruct((n_micro, width, per), BF16),
        jax.ShapeDtypeStruct((10, 1, width), F32),
        jax.ShapeDtypeStruct((10, 1, width), F32),
        jax.ShapeDtypeStruct((1, 800), F32),
    )
    low = pltpu.VMEM((total, width), BF16)
    message = pltpu.VMEM((CHUNKS, total // CHUNKS * width // 128, 128), BF16)
    wide = pltpu.VMEM((total, 384), BF16)
    dma = pltpu.SemaphoreType.DMA
    held = pl.pallas_call(
        kernel,
        out_shape=tuple(pltpu.VMEM(s.shape, s.dtype) for s in shapes),
        in_specs=[pl.BlockSpec(memory_space=pl.ANY)] * 7,
        out_specs=(pl.BlockSpec(memory_space=pltpu.VMEM),) * 4,
        scratch_shapes=[
            pltpu.VMEM((n_micro, width, per), BF16),
            pltpu.VMEM(timesteps.shape, jnp.int32),
            pltpu.VMEM((width, time_table.shape[0]), BF16),
            pltpu.VMEM((width, width), BF16),
            pltpu.VMEM((width, hidden), BF16),
            pltpu.VMEM((width, hidden), BF16),
            pltpu.VMEM((n_micro, width, per), BF16),
            dma((7,)),
            pltpu.VMEM((total, hidden), F32),
            message,
            message,
            message,
            pltpu.VMEM((total, width), F32),
            low,
            low,
            message,
            message,
            message,
            pltpu.VMEM((total, width), F32),
            pltpu.VMEM((total, 128), F32),
            pltpu.VMEM((total, hidden), F32),
            wide,
            wide,
            pltpu.VMEM((4, total, 384), BF16),
            pltpu.VMEM((4, total, 384), BF16),
            pltpu.VMEM((hidden, width), BF16),
            pltpu.VMEM((width, width), BF16),
            pltpu.VMEM((384, width), BF16),
            pltpu.VMEM((hidden, width), BF16),
            pltpu.VMEM((hidden, width), BF16),
            pltpu.VMEM((width, 4 * total), BF16),
            pltpu.VMEM((4, total, width), F32),
            pltpu.VMEM((width, 4 * total), BF16),
            pltpu.VMEM((256, total), BF16),
            pltpu.VMEM((256, total), BF16),
            pltpu.VMEM((2, 2, 64, lanes), BF16),
            pltpu.VMEM((2, 64, lanes), BF16),
            pltpu.VMEM((2, 4, FF_ROWS, lanes), BF16),
            pltpu.VMEM((2, 2, FF_ROWS, lanes), BF16),
            pltpu.VMEM((2, FF_ROWS, lanes), BF16),
            pltpu.VMEM((2, 4, PIECE, lanes), BF16),
            pltpu.VMEM((7, PIECE, lanes), BF16),
            pltpu.VMEM((8, 64, 128), BF16),
            pltpu.VMEM((7, 64, 128), BF16),
        ]
        + [dma((CHUNKS,))] * 6
        + [dma((3,))] * 2
        + [dma((3,))] * 2
        + [dma((CHUNKS,))]
        + [dma((1,))] * 2
        + [dma((2, 2))] * 2
        + [dma((1,))] * 2
        + [dma((2,))] * 2
        + [dma((1,))] * 2,
        compiler_params=pltpu.CompilerParams(collective_id=0, has_side_effects=True),
    )(
        jnp.swapaxes(saved_inputs[0], 1, 2),
        timesteps,
        time_table.T,
        skip_weight[0],
        ff_in[0].T,
        ff_out[0].T,
        jnp.swapaxes(output_cotangent, 1, 2),
    )
    grads, d_in, d_out, d_skip = pl.pallas_call(
        finish,
        out_shape=shapes,
        in_specs=[pl.BlockSpec(memory_space=pltpu.VMEM)] * 4,
        out_specs=(pl.BlockSpec(memory_space=pl.ANY),) * 4,
        scratch_shapes=[dma((4,))],
        compiler_params=pltpu.CompilerParams(vmem_limit_bytes=2**20),
    )(*held)
    grads = jnp.swapaxes(grads, 1, 2)[None]
    return (grads, d_skip, jnp.swapaxes(d_in, 0, 1), jnp.swapaxes(d_out, 0, 1))


def solution(mesh):
    split = Mesh(
        mesh.devices.reshape(mesh.shape["section"], 8, 4, 2, 2), ("section", "z", "x", "w", "core")
    )
    return jax.shard_map(
        shards,
        mesh=split,
        in_specs=(
            P("section", None, DP, None),
            P(None, DP),
            P(),
            P("section", None, None),
            P("section", None, None),
            P("section", None, None),
            P(None, DP, None),
        ),
        out_specs=(
            P("section", None, DP, None),
            P("section", DP),
            P("section", DP, None),
            P("section", DP, None),
        ),
        check_vma=False,
    )
```

```python
import jax
import jax.numpy as jnp
from jax import lax
from jax.experimental import pallas as pl
from jax.experimental.pallas import tpu as pltpu
from jax.sharding import Mesh
from jax.sharding import PartitionSpec as P

DP = ("z", "x", "w", "core")
MESH = pl.DeviceIdType.MESH
EPS = 1e-06
CHUNKS = 8
LAG = 5
FF_ROWS = 40
PIECE = 16
F32 = jnp.float32
BF16 = jnp.bfloat16


def dot(left, right):
    return jnp.dot(left, right, preferred_element_type=F32)


def dot_nt(left, right):
    return lax.dot_general(left, right, (((1,), (1,)), ((), ())), preferred_element_type=F32)


def kernel(
    xt_hbm,
    ts_hbm,
    tablet_hbm,
    wskip_hbm,
    wint_hbm,
    woutt_hbm,
    cott_hbm,
    grads_ref,
    din_ref,
    dout_ref,
    dskip_ref,
    xt_ref,
    ts_ref,
    tablet_ref,
    wskip_ref,
    wint_ref,
    woutt_ref,
    cott_ref,
    in_sem,
    ga_buf,
    v_msg,
    g_msg,
    k_msg,
    x_buf,
    z_buf,
    g_buf,
    vsend,
    csend,
    ksend,
    u_buf,
    r_buf,
    ds_buf,
    ch_buf,
    chsh_buf,
    nq,
    gq,
    sel,
    win_q,
    wout_q,
    win_n,
    wout_n,
    act_t,
    ds_q,
    gpre_t,
    za_t,
    zb_t,
    skip_part,
    skip_core,
    part,
    r_x1,
    r_x2,
    own_skip,
    r_own,
    z_send,
    r_z,
    vs_sem,
    vr_sem,
    cs_sem,
    cr_sem,
    ks_sem,
    kr_sem,
    n_s,
    n_r,
    gs_s,
    gs_r,
    gw_r,
    sk_s,
    sk_r,
    x1_s,
    x1_r,
    own_s,
    own_r,
    x2_s,
    x2_r,
    z_s,
    z_r,
):
    section = lax.axis_index("section")
    mz = lax.axis_index("z")
    mx = lax.axis_index("x")
    mw = lax.axis_index("w")
    mc = lax.axis_index("core")
    pairs = (
        (ts_hbm, ts_ref),
        (tablet_hbm, tablet_ref),
        (xt_hbm, xt_ref),
        (wskip_hbm, wskip_ref),
        (wint_hbm, wint_ref),
        (woutt_hbm, woutt_ref),
        (cott_hbm, cott_ref),
    )
    loads = [pltpu.make_async_copy(a, b, in_sem.at[i]) for i, (a, b) in enumerate(pairs)]
    for load in loads:
        load.start()
    micro, width, per = xt_ref.shape
    total = micro * per
    rows = total // CHUNKS
    levels = tablet_ref.shape[1]
    hidden = wint_ref.shape[1]

    def remote(src, dst, send, recv, device):
        return pltpu.make_async_remote_copy(
            src_ref=src,
            dst_ref=dst,
            send_sem=send,
            recv_sem=recv,
            device_id=device,
            device_id_type=MESH,
        )

    x_near = mx + 1 - 2 * lax.rem(mx, 2)
    x_far = 3 - mx
    x_op = lax.rem(mx + 2, 4)

    barrier = pltpu.get_barrier_semaphore()
    greet = [{"section": lax.rem(section + step, 4)} for step in (1, 3)]
    greet += [{"core": 1 - mc}, {"x": x_near}, {"x": x_far}, {"x": x_op}, {"w": 1 - mw}]
    greet += [{"w": 1 - mw, "x": to} for to in (x_near, x_far, x_op)]
    greet += [{"z": lax.rem(mz + step, 8)} for step in range(1, 8)]
    for device in greet:
        pl.semaphore_signal(barrier, inc=1, device_id=device, device_id_type=MESH)

    def at(c):
        if isinstance(c, int):
            return slice(c * rows, (c + 1) * rows)
        return pl.ds(pl.multiple_of(c * rows, rows), rows)

    def value_copy(c):
        device = {"section": 3 - section}
        return remote(vsend.at[c], v_msg.at[c], vs_sem.at[c], vr_sem.at[c], device)

    def chain_copy(c):
        device = {"section": lax.rem(section + 3, 4)}
        return remote(csend.at[c], g_msg.at[c], cs_sem.at[c], cr_sem.at[c], device)

    def skip_copy(c):
        device = {"section": lax.rem(section + 1, 4)}
        return remote(ksend.at[c], k_msg.at[c], ks_sem.at[c], kr_sem.at[c], device)

    def paced(copy, c):
        @pl.when(c >= 2)
        def _():
            copy(c - 2).wait_send()

        copy(c).start()

    rest = width - 256
    short = rows // 2

    def pack(buf, c, value):
        value = value.astype(BF16)
        buf[c, 0:rows, :] = value[:, 0:128]
        buf[c, rows : 2 * rows, :] = value[:, 128:256]
        buf[c, 2 * rows :, 0:rest] = value[0:short, 256:width]
        buf[c, 2 * rows :, rest:] = value[short:, 256:width]

    def unpack(buf, c):
        tail = jnp.concatenate([buf[c, 2 * rows :, 0:rest], buf[c, 2 * rows :, rest:]], axis=0)
        return jnp.concatenate([buf[c, 0:rows, :], buf[c, rows : 2 * rows, :], tail], axis=1)

    def front(c, z):
        united = x_buf[at(c), :] + dot(z, wskip_ref[...])
        recip = lax.rsqrt(jnp.mean(united * united, axis=-1, keepdims=True) + EPS)
        normed = (united * recip).astype(BF16)
        preact = dot(normed, wint_ref[...])
        sigma = jax.nn.sigmoid(preact)
        return united, recip, normed, preact, sigma, sigma * (1.0 + preact * (1.0 - sigma))

    def keep(c, united, recip, normed, slope):
        here = at(c)
        u_buf[here, :] = united
        r_buf[here, :] = jnp.broadcast_to(recip, (rows, 128))
        nq[me, here, 0:width] = normed
        ds_buf[here, :] = slope

    def encode(c):
        united, recip, normed, preact, sigma, slope = front(c, z_buf[at(c), :])
        active = (preact * sigma).astype(BF16)
        pack(vsend, c, united + dot(active, wout_n[...]))
        paced(value_copy, c)
        keep(c, united, recip, normed, slope)

    def back(gy, gact, united, recip, slope):
        pre = (gact * slope).astype(BF16)
        gn = dot(pre, win_n[...])
        mean = jnp.mean(gn * united, axis=-1, keepdims=True)
        chain = gy + recip * gn - united * (recip * recip * recip * mean)
        return chain.astype(BF16)

    def keep_chain(c, chain):
        here = at(c)
        ch_buf[here, 0:width] = chain
        chsh_buf[here, 64 : 64 + width] = chain

    def backward(c, which):
        here = at(c)
        chain_copy(c).wait_recv()
        if which == 1:

            @pl.when(c >= 3)
            def _():
                chain_copy(c - 3).wait_send()

        gy = unpack(g_msg, c).astype(F32)
        if which == 0:
            skip_copy(c).wait_recv()
            gy = gy + unpack(k_msg, c).astype(F32)
        low = gy.astype(BF16)
        gq[me, here, 64 : 64 + width] = low
        if which == 0:
            share(c)
        gact = dot(low, woutt_ref[...])
        chain = back(gy, gact, u_buf[here, :], r_buf[here, 0:1], ds_buf[here, :])
        if which == 1:
            pack(csend, c, chain)
            chain_copy(c).start()
        keep_chain(c, chain)

    def when(condition, action):
        pl.when(condition)(action)

    def step2_front(f):
        value_copy(f).wait_recv()
        z = unpack(v_msg, f)
        united, recip, normed, _, _, slope = front(f, z)
        z_buf[at(f), :] = z
        keep(f, united, recip, normed, slope)

    def step2_back(b):
        chain_copy(b).wait_recv()
        when(b >= 3, lambda: chain_copy(b - 3).wait_send())
        here = at(b)
        low = unpack(g_msg, b)
        gact = dot(low, woutt_ref[...])
        chain = back(low.astype(F32), gact, u_buf[here, :], r_buf[here, 0:1], ds_buf[here, :])
        joint = chain.astype(F32) + dot_nt(chain, wskip_ref[...]).astype(BF16).astype(F32)
        pack(csend, b, joint)
        chain_copy(b).start()
        gq[me, here, 64 : 64 + width] = low
        keep_chain(b, chain)

    def step3(c):
        here = at(c)
        value_copy(c).wait_recv()
        when(c >= 3, lambda: chain_copy(c - 3).wait_send())
        when(c >= 2, lambda: skip_copy(c - 2).wait_send())
        z = unpack(v_msg, c)
        united, recip, normed, _, _, slope = front(c, z)
        chain = back(g_buf[here, :].astype(F32), ga_buf[here, :], united, recip, slope)
        pack(csend, c, chain)
        chain_copy(c).start()
        pack(ksend, c, dot_nt(chain, wskip_ref[...]))
        skip_copy(c).start()
        z_buf[here, :] = z
        nq[me, here, 0:width] = normed
        keep_chain(c, chain)

    me = 2 * mw + mc
    mates = (2 * mw + 1 - mc, 2 * (1 - mw) + mc, 2 * (1 - mw) + 1 - mc)
    towards = ({"core": 1 - mc}, {"w": 1 - mw}, {"core": 1 - mc})

    def share_n(to):
        slot = mates[1] if to == 2 else me
        return remote(nq.at[slot], nq.at[slot], n_s.at[to], n_r.at[to], towards[to])

    def share_g(c, to):
        slot = mates[1] if to == 2 else me
        block = gq.at[slot, at(c)]
        got = gw_r.at[c] if to == 1 else gs_r.at[to]
        return remote(block, block, gs_s.at[to], got, towards[to])

    def whole_g(to):
        block = gq.at[me if to < 2 else mates[1]]
        return remote(block, block, gs_s.at[to], gs_r.at[to], towards[to])

    def share(c):
        for to in range(2):
            share_g(c, to).start()

    def share_normed():
        for to in range(2):
            share_n(to).start()

    nq[me, :, width:] = jnp.zeros((total, 384 - width), BF16)
    gq[me, :, 0:64] = jnp.zeros((total, 64), BF16)
    ch_buf[:, width:] = jnp.zeros((total, 384 - width), BF16)
    chsh_buf[:, 0:64] = jnp.zeros((total, 64), BF16)

    def rows_of(m):
        return slice(m * per, (m + 1) * per)

    def choose_units():
        line = lax.broadcasted_iota(jnp.int32, (hidden, width), 1)
        unit = 40 * (4 * (lax.rem(line, 80) // 10) + line // 80) + 10 * me + lax.rem(line, 10)
        chosen = lax.broadcasted_iota(jnp.int32, (hidden, width), 0) == unit
        sel[...] = jnp.where(chosen, 1.0, 0.0).astype(BF16)
        win_q[...] = dot(wint_ref[...], sel[...]).astype(BF16)
        wout_q[0:64, :] = jnp.zeros((64, width), BF16)
        wout_q[64:, :] = dot(woutt_ref[...], sel[...]).astype(BF16)

    def embed(m):
        onehot = ts_ref[m : m + 1, :] == lax.broadcasted_iota(jnp.int32, (levels, per), 0)
        rows_t = dot(tablet_ref[...], jnp.where(onehot, 1.0, 0.0).astype(BF16))
        z_buf[rows_of(m), :] = rows_t.T.astype(BF16)

    for load in loads[0:3]:
        load.wait()

    @pl.when(section < 2)
    def _():
        for m in range(micro):
            embed(m)

    for m in range(micro):
        x_buf[rows_of(m), :] = xt_ref[m].astype(F32).T
    for load in loads[3:]:
        load.wait()

    @pl.when(section == 3)
    def _():
        for m in range(micro):
            cot = cott_ref[m].astype(F32).T.astype(BF16)
            g_buf[rows_of(m), :] = cot
            gq[me, rows_of(m), 64 : 64 + width] = cot
        ga_buf[...] = dot(g_buf[...], woutt_ref[...])

    @pl.when(section < 2)
    def _():
        wout_n[...] = woutt_ref[...].T

    @pl.when(section >= 2)
    def _():
        win_n[...] = wint_ref[...].T

    pl.semaphore_wait(barrier, len(greet))

    @pl.when(section < 2)
    def _():
        @pl.loop(0, CHUNKS)
        def _(c):
            encode(c)

        share_normed()
        win_n[...] = wint_ref[...].T
        choose_units()

    @pl.when(section == 3)
    def _():
        @pl.loop(0, CHUNKS)
        def _(c):
            share(c)

        choose_units()

        @pl.loop(0, CHUNKS)
        def _(c):
            step3(c)

        share_normed()

    @pl.when(section == 2)
    def _():
        choose_units()

        @pl.loop(0, LAG)
        def _(t):
            step2_front(t)

        @pl.loop(0, CHUNKS)
        def _(t):
            step2_back(t)

            @pl.when(t < CHUNKS - LAG)
            def _():
                step2_front(t + LAG)

        share_normed()

    slot = lax.broadcasted_iota(jnp.int32, (256, width), 0)
    channel = lax.broadcasted_iota(jnp.int32, (256, width), 1)
    third = lax.rem(slot, 2)
    pixel = lax.rem(slot, 64) // 2
    first = 10 * (4 * lax.rem(pixel, 8) + pixel // 8) + 5 * lax.rem(slot // 64, 2)
    first = first + 2 * (slot // 128)
    for dst, pick in (
        (za_t, channel == first + 2 * third),
        (zb_t, (channel == first + 1) & (third == 0)),
    ):
        dst[...] = dot_nt(jnp.where(pick, 1.0, 0.0).astype(BF16), z_buf[...]).astype(BF16)

    share_n(1).wait_recv()
    share_n(2).start()
    share_n(0).wait_recv()
    share_n(2).wait_recv()

    @pl.loop(0, 4)
    def _(q):
        preact = dot(nq[q, :, 0:width], win_q[...])
        sigma = jax.nn.sigmoid(preact)
        ds_q[q] = sigma * (1.0 + preact * (1.0 - sigma))
        act_t[:, pl.ds(pl.multiple_of(q * total, total), total)] = (preact * sigma).astype(BF16).T

    for which in (0, 1):

        @pl.when(section == which)
        def _():
            @pl.loop(0, CHUNKS)
            def _(c):
                backward(c, which)

    def joined(left, right):
        return left[:, 0:256], left[:, 256:384] + right[:, 0:128], right[:, 128:384]

    edges = (slice(0, 256), slice(256, 384), slice(384, 640))

    @pl.when((section == 1) | (section == 2))
    def _():
        @pl.loop(0, CHUNKS)
        def _(c):
            share(c)

    skips = joined(dot(za_t[...], ch_buf[...]), dot(zb_t[...], chsh_buf[...]))
    for edge, value in zip(edges, skips):
        skip_part[:, :, :, edge] = value.astype(BF16).reshape(2, 2, 64, -1)
    skip1 = remote(skip_part.at[1 - mc], skip_core, sk_s.at[0], sk_r.at[0], {"core": 1 - mc})
    skip1.start()

    def own_copy(k):
        v = 1 - mw if k % 2 else mw
        to = (mx, x_near, x_far, x_op)[k // 2]
        return remote(own_skip.at[v, to], r_own.at[k - 1], own_s.at[0], own_r.at[0], {"w": v, "x": to})


    def through(q):
        pre = (dot(gq[q], wout_q[...]) * ds_q[q]).astype(BF16)
        gpre_t[:, pl.ds(pl.multiple_of(q * total, total), total)] = pre.T

    def pass_on():
        @pl.loop(0, CHUNKS)
        def _(c):
            share_g(c, 1).wait_recv()
            share_g(c, 2).start()

    when(mw == 0, pass_on)
    through(me)
    whole_g(0).wait_recv()
    through(mates[0])
    when(mw == 1, pass_on)
    skip1.wait_recv()
    for v in range(2):
        mine = skip_part[mc, v].astype(F32) + skip_core[v].astype(F32)
        own_skip[v] = mine.astype(BF16).reshape(4, PIECE, 2 * width)
    through(mates[1])
    whole_g(2).wait_recv()
    through(mates[2])

    everyone = 4 * total
    d_out = dot(act_t[...], gq[...].reshape(everyone, 384))
    d_in = dot(gpre_t[...], nq[...].reshape(everyone, 384))
    for edge, value in zip(edges, joined(d_in, d_out)):
        value = value.astype(BF16).reshape(4, 2, FF_ROWS, -1)
        for color in range(2):
            part[color, :, :, edge] = value[:, color]

    def x1_copy(color, k):
        device = x_far if color else x_near
        block = device if k == 0 else x_op
        src, dst = part.at[color, block], r_x1.at[color, k]
        return remote(src, dst, x1_s.at[color, k], x1_r.at[color, k], {"x": device})

    def x2_copy(color):
        device = x_near if color else x_far
        src = part.at[color, device]
        return remote(src, r_x2.at[color], x2_s.at[color], x2_r.at[color], {"x": device})

    for k in (1, 0):
        for color in range(2):
            x1_copy(color, k).start()
    for k in range(7, 0, -1):
        own_copy(k).start()
    for m in range(micro):
        grads_ref[m] = ch_buf[m * per : (m + 1) * per, 0:width].astype(F32).T.astype(BF16)

    def added(left, right):
        return left.astype(F32) + right.astype(F32)

    for k in (1, 0):
        for color in range(2):
            x1_copy(color, k).wait_recv()
            block = mx if k == 0 else (x_near if color else x_far)
            part[color, block] = added(part[color, block], r_x1[color, k]).astype(BF16)
            if k == 1:
                x2_copy(color).start()

    def z_copy(k):
        target = lax.rem(mz + k, 8)
        return remote(z_send.at[target], r_z.at[k - 1], z_s.at[0], z_r.at[0], {"z": target})

    for to in range(3):
        share_n(to).wait_send()
    skip1.wait_send()

    for to in range(3):
        whole_g(to).wait_send()

    @pl.when(section < 2)
    def _():
        for late in range(1, 3):
            value_copy(CHUNKS - late).wait_send()

    @pl.when(section > 0)
    def _():
        for late in range(1, 4):
            chain_copy(CHUNKS - late).wait_send()

    @pl.when(section == 3)
    def _():
        for late in range(1, 3):
            skip_copy(CHUNKS - late).wait_send()

    tails = own_skip[mw, mx].astype(F32)
    all_own = remote(r_own, r_own, own_s.at[0], own_r.at[0], {"w": 1 - mw})
    all_own.wait_recv()
    for k in range(7):
        tails = tails + r_own[k].astype(F32)
    for color in range(2):
        x2_copy(color).wait_recv()
        block = added(part[color, mx], r_x2[color])
        for j in range(4):
            piece = (block[10 * j : 10 * j + 10], tails[8 * color + 2 * j : 8 * color + 2 * j + 2])
            piece = jnp.concatenate(piece, axis=0)
            stack = [piece[:, 128 * t : 128 * t + 128] for t in range(5)]
            stack = jnp.concatenate(stack + [jnp.zeros((4, 128), F32)], axis=0)
            z_send[4 * color + j] = stack.astype(BF16)
    far_first = (4, 3, 5, 2, 6, 1, 7)
    for k in far_first:
        z_copy(k).start()
    acc = z_send[mz].astype(F32)
    all_z = remote(r_z, r_z, z_s.at[0], z_r.at[0], {"z": lax.rem(mz + 1, 8)})
    all_z.wait_recv()
    for k in range(7):
        acc = acc + r_z[k].astype(F32)
    acc = jnp.concatenate([acc[12 * t : 12 * t + 12] for t in range(5)], axis=1)

    for j in range(10):
        din_ref[j] = acc[j : j + 1, 0:width]
        dout_ref[j] = acc[j : j + 1, width:]
    half = width // 2
    lead, mid, last = acc[10:11, 0:width], acc[10:11, width:], acc[11:12, 0:width]

    @pl.when(mc == 0)
    def _():
        dskip_ref[:, 0:width] = lead
        dskip_ref[:, width : 2 * width] = mid
        dskip_ref[:, 2 * width :] = last[:, 0:half]

    @pl.when(mc == 1)
    def _():
        dskip_ref[:, 0:half] = lead[:, half:]
        dskip_ref[:, half : half + width] = mid
        dskip_ref[:, half + width :] = last

    for color in range(2):
        for k in range(2):
            x1_copy(color, k).wait_send()
        x2_copy(color).wait_send()
    all_own.wait_send()
    all_z.wait_send()


def finish(*refs):
    copies = [pltpu.make_async_copy(refs[i], refs[4 + i], refs[8].at[i]) for i in range(4)]
    for copy in copies:
        copy.start()
    for copy in copies:
        copy.wait()


def shards(saved_inputs, timesteps, time_table, skip_weight, ff_in, ff_out, output_cotangent):
    n_micro, per, width = saved_inputs.shape[1:]
    hidden = ff_in.shape[1]
    total = n_micro * per
    lanes = 2 * width
    shapes = (
        jax.ShapeDtypeStruct((n_micro, width, per), BF16),
        jax.ShapeDtypeStruct((10, 1, width), F32),
        jax.ShapeDtypeStruct((10, 1, width), F32),
        jax.ShapeDtypeStruct((1, 800), F32),
    )
    low = pltpu.VMEM((total, width), BF16)
    message = pltpu.VMEM((CHUNKS, total // CHUNKS * width // 128, 128), BF16)
    wide = pltpu.VMEM((total, 384), BF16)
    dma = pltpu.SemaphoreType.DMA
    held = pl.pallas_call(
        kernel,
        out_shape=tuple(pltpu.VMEM(s.shape, s.dtype) for s in shapes),
        in_specs=[pl.BlockSpec(memory_space=pl.ANY)] * 7,
        out_specs=(pl.BlockSpec(memory_space=pltpu.VMEM),) * 4,
        scratch_shapes=[
            pltpu.VMEM((n_micro, width, per), BF16),
            pltpu.VMEM(timesteps.shape, jnp.int32),
            pltpu.VMEM((width, time_table.shape[0]), BF16),
            pltpu.VMEM((width, width), BF16),
            pltpu.VMEM((width, hidden), BF16),
            pltpu.VMEM((width, hidden), BF16),
            pltpu.VMEM((n_micro, width, per), BF16),
            dma((7,)),
            pltpu.VMEM((total, hidden), F32),
            message,
            message,
            message,
            pltpu.VMEM((total, width), F32),
            low,
            low,
            message,
            message,
            message,
            pltpu.VMEM((total, width), F32),
            pltpu.VMEM((total, 128), F32),
            pltpu.VMEM((total, hidden), F32),
            wide,
            wide,
            pltpu.VMEM((4, total, 384), BF16),
            pltpu.VMEM((4, total, 384), BF16),
            pltpu.VMEM((hidden, width), BF16),
            pltpu.VMEM((width, width), BF16),
            pltpu.VMEM((384, width), BF16),
            pltpu.VMEM((hidden, width), BF16),
            pltpu.VMEM((hidden, width), BF16),
            pltpu.VMEM((width, 4 * total), BF16),
            pltpu.VMEM((4, total, width), F32),
            pltpu.VMEM((width, 4 * total), BF16),
            pltpu.VMEM((256, total), BF16),
            pltpu.VMEM((256, total), BF16),
            pltpu.VMEM((2, 2, 64, lanes), BF16),
            pltpu.VMEM((2, 64, lanes), BF16),
            pltpu.VMEM((2, 4, FF_ROWS, lanes), BF16),
            pltpu.VMEM((2, 2, FF_ROWS, lanes), BF16),
            pltpu.VMEM((2, FF_ROWS, lanes), BF16),
            pltpu.VMEM((2, 4, PIECE, lanes), BF16),
            pltpu.VMEM((7, PIECE, lanes), BF16),
            pltpu.VMEM((8, 64, 128), BF16),
            pltpu.VMEM((7, 64, 128), BF16),
        ]
        + [dma((CHUNKS,))] * 6
        + [dma((3,))] * 2
        + [dma((3,))] * 2
        + [dma((CHUNKS,))]
        + [dma((1,))] * 2
        + [dma((2, 2))] * 2
        + [dma((1,))] * 2
        + [dma((2,))] * 2
        + [dma((1,))] * 2,
        compiler_params=pltpu.CompilerParams(collective_id=0, has_side_effects=True),
    )(
        jnp.swapaxes(saved_inputs[0], 1, 2),
        timesteps,
        time_table.T,
        skip_weight[0],
        ff_in[0].T,
        ff_out[0].T,
        jnp.swapaxes(output_cotangent, 1, 2),
    )
    grads, d_in, d_out, d_skip = pl.pallas_call(
        finish,
        out_shape=shapes,
        in_specs=[pl.BlockSpec(memory_space=pltpu.VMEM)] * 4,
        out_specs=(pl.BlockSpec(memory_space=pl.ANY),) * 4,
        scratch_shapes=[dma((4,))],
        compiler_params=pltpu.CompilerParams(vmem_limit_bytes=2**20),
    )(*held)
    grads = jnp.swapaxes(grads, 1, 2)[None]
    return (grads, d_skip, jnp.swapaxes(d_in, 0, 1), jnp.swapaxes(d_out, 0, 1))


def solution(mesh):
    split = Mesh(
        mesh.devices.reshape(mesh.shape["section"], 8, 4, 2, 2), ("section", "z", "x", "w", "core")
    )
    return jax.shard_map(
        shards,
        mesh=split,
        in_specs=(
            P("section", None, DP, None),
            P(None, DP),
            P(),
            P("section", None, None),
            P("section", None, None),
            P("section", None, None),
            P(None, DP, None),
        ),
        out_specs=(
            P("section", None, DP, None),
            P("section", DP),
            P("section", DP, None),
            P("section", DP, None),
        ),
        check_vma=False,
    )
```
